8 devices in a mesh: data: 1 (over z), stage: 8 (over y, x, core).
Axes of the slice: x: 2, y: 2, z: 1, core: 2. Of those that a mesh axis runs over, the one named last changes fastest.
Arguments:
- x: bfloat16 [1, 512, 1280], P('data')
- y: bfloat16 [1, 512, 1280], P('data')
- w_qkv: bfloat16 [8, 1280, 3840], P('stage')
- w_out: bfloat16 [8, 1280, 1280], P('stage')
- w_up: bfloat16 [8, 1280, 5120], P('stage')
- w_down: bfloat16 [8, 5120, 1280], P('stage')
- norm_gain: bfloat16 [8, 2, 1280], P('stage')
Outputs:
- output 1: float32 [1], P('data')
- output 2: float32 [8, 1280, 3840], P(('data', 'stage'))
- output 3: float32 [8, 1280, 1280], P(('data', 'stage'))
- output 4: float32 [8, 1280, 5120], P(('data', 'stage'))
- output 5: float32 [8, 5120, 1280], P(('data', 'stage'))
- output 6: float32 [8, 2, 1280], P(('data', 'stage'))
All inputs are finite; a program needn't handle non-finite values.
Results may differ from the reference program's by a relative error of at most 0.0141127.
Values are sent between devices in bfloat16 or wider.
A program may use at most 1 GiB of HBM per device.

```python
import jax
import jax.numpy as jnp
from jax import lax

DIM = 1280
HEADS = 20
SEQ = 512
LAYERS = 8
BLOCK = 256
FFN = 4 * DIM
HEAD_DIM = DIM // HEADS
EPS = 1e-6


def setup_inputs(seed: int = 0, part: int = 0) -> dict:
    base_key = jax.random.key(seed)
    part_key = jax.random.fold_in(base_key, part)
    key_x, key_y = jax.random.split(part_key)
    weight_keys = jax.random.split(base_key, 5)
    x = jax.random.normal(key_x, (1, SEQ, DIM), jnp.float32).astype(jnp.bfloat16)
    y = jax.random.normal(key_y, (1, SEQ, DIM), jnp.float32).astype(jnp.bfloat16)
    w_qkv = (jax.random.normal(weight_keys[0], (LAYERS, DIM, 3 * DIM), jnp.float32) * DIM ** -0.5).astype(jnp.bfloat16)
    w_out = (jax.random.normal(weight_keys[1], (LAYERS, DIM, DIM), jnp.float32) * DIM ** -0.5).astype(jnp.bfloat16)
    w_up = (jax.random.normal(weight_keys[2], (LAYERS, DIM, FFN), jnp.float32) * DIM ** -0.5).astype(jnp.bfloat16)
    w_down = (jax.random.normal(weight_keys[3], (LAYERS, FFN, DIM), jnp.float32) * FFN ** -0.5).astype(jnp.bfloat16)
    norm_gain = (1.0 + 0.3 * jax.random.normal(weight_keys[4], (LAYERS, 2, DIM), jnp.float32)).astype(jnp.bfloat16)
    return {'x': x, 'y': y, 'w_qkv': w_qkv, 'w_out': w_out, 'w_up': w_up, 'w_down': w_down, 'norm_gain': norm_gain}


def rms_norm(hidden, gain):
    hid_f = hidden.astype(jnp.float32)
    inv_rms = lax.rsqrt(jnp.mean(hid_f * hid_f, axis=-1, keepdims=True) + EPS)
    return (hid_f * inv_rms * gain.astype(jnp.float32)).astype(jnp.bfloat16)


def causal_attention(qkv_all):
    seq_len = qkv_all.shape[0]
    num_blocks = seq_len // BLOCK
    queries = qkv_all[:, :DIM].reshape(num_blocks, BLOCK, HEADS, HEAD_DIM)
    keys_all = qkv_all[:, DIM:2 * DIM].reshape(seq_len, HEADS, HEAD_DIM).astype(jnp.float32)
    values_all = qkv_all[:, 2 * DIM:].reshape(seq_len, HEADS, HEAD_DIM).astype(jnp.float32)
    key_pos = jnp.arange(seq_len)

    def one_block(operands):
        q_block, block_idx = operands
        scores = jnp.einsum('qhd,khd->hqk', q_block.astype(jnp.float32), keys_all) * HEAD_DIM ** -0.5
        query_pos = block_idx * BLOCK + jnp.arange(BLOCK)
        causal_mask = key_pos[None, :] <= query_pos[:, None]
        scores = jnp.where(causal_mask[None], scores, -1e30)
        probs_bf = jax.nn.softmax(scores, axis=-1).astype(jnp.bfloat16)
        att_out = jnp.einsum('hqk,khd->qhd', probs_bf.astype(jnp.float32), values_all)
        return att_out.astype(jnp.bfloat16)

    blocks_out = lax.map(one_block, (queries, jnp.arange(num_blocks)))
    return blocks_out.reshape(seq_len, DIM)


def layer_step(hidden, layer_params):
    w_qkv, w_out, w_up, w_down, norm_gain = layer_params
    normed = rms_norm(hidden, norm_gain[0])
    qkv_all = jnp.dot(normed, w_qkv, preferred_element_type=jnp.float32).astype(jnp.bfloat16)
    att_mix = causal_attention(qkv_all)
    hidden = (hidden.astype(jnp.float32) + jnp.dot(att_mix, w_out, preferred_element_type=jnp.float32)).astype(jnp.bfloat16)
    normed = rms_norm(hidden, norm_gain[1])
    upper = jnp.dot(normed, w_up, preferred_element_type=jnp.float32)
    act_bf = jax.nn.gelu(upper).astype(jnp.bfloat16)
    return (hidden.astype(jnp.float32) + jnp.dot(act_bf, w_down, preferred_element_type=jnp.float32)).astype(jnp.bfloat16)


def model_loss(params, x, y):
    def scan_body(hidden, layer_params):
        return jax.checkpoint(layer_step)(hidden, layer_params), None
    h_final, scan_rest = lax.scan(scan_body, x[0], params)
    resid_err = h_final.astype(jnp.float32) - y[0].astype(jnp.float32)
    return 0.5 * jnp.mean(resid_err * resid_err)


def reference(x, y, w_qkv, w_out, w_up, w_down, norm_gain):
    params = (w_qkv, w_out, w_up, w_down, norm_gain)
    loss_val, grads = jax.value_and_grad(model_loss)(params, x, y)
    return (loss_val.reshape(1), grads[0].astype(jnp.float32), grads[1].astype(jnp.float32), grads[2].astype(jnp.float32), grads[3].astype(jnp.float32), grads[4].astype(jnp.float32))
```

```python
import functools
import math

import jax
import jax.numpy as jnp
from jax import lax
from jax.experimental import pallas as pl
from jax.experimental.pallas import tpu as pltpu
from jax.sharding import PartitionSpec as P

MESH = pl.DeviceIdType.MESH
BF = jnp.bfloat16
F32 = jnp.float32
HEAD_DIM = 64
ROWS = 256
EPS = 1e-6
GELU_C = math.sqrt(2.0 / math.pi)
GELU_A = 0.044715
LOG2E = math.log2(math.e)


def dot_nn(a, b):
    return jnp.dot(a, b, preferred_element_type=F32)


def dot_nt(a, b):
    return lax.dot_general(a, b, (((1,), (1,)), ((), ())), preferred_element_type=F32)


def dot_tn(a, b):
    return lax.dot_general(a, b, (((0,), (0,)), ((), ())), preferred_element_type=F32)


def norm_stats(h_bf):
    h = h_bf.astype(F32)
    inv = lax.rsqrt(jnp.mean(h * h, axis=-1, keepdims=True) + EPS)
    return h, inv


def norm_grad(dn, h_bf, gain):
    h, inv = norm_stats(h_bf)
    hhat = h * inv
    dgain = jnp.sum(dn * hhat, axis=0, keepdims=True)
    dhhat = dn * gain
    corr = jnp.mean(dhhat * hhat, axis=-1, keepdims=True)
    return inv * (dhhat - hhat * corr), dgain


def gelu_parts(u):
    u2 = u * u
    t = jnp.tanh(u * (GELU_C + (GELU_C * GELU_A) * u2))
    return u2, t


def pipeline_kernel(stages, seq, width, x_ref, y_ref, wqkv, wout, wup, wdown, gain_ref,
                    loss_ref, dgain_ref, n1_o, a_o, n2_o, act_o, du_o, dqkv_o, dhm_o, dho_o,
                    ring, hin, hs, hmid, n1, att, n2, qkv, u_buf, act, acc, dho, dhs, dhm, da, du, dqkv, dkv, bias, loss_in,
                    wsem, xsem, osem, fs, fr, bs, br, ls, lr):
    me = lax.axis_index('stage')
    data = lax.axis_index('data')
    last = stages - 1
    right = lax.rem(me + 1, stages)
    left = lax.rem(me + stages - 1, stages)
    D = width
    CH = D
    pairs = D // (2 * HEAD_DIM)
    ffn_chunks = wup.shape[2] // CH
    count = float(seq * width)

    def src(kind, j):
        cols = pl.ds(pl.multiple_of(j * CH, CH), CH)
        if kind == 'q':
            return wqkv.at[0, :, cols]
        if kind == 'o':
            return wout.at[0]
        if kind == 'u':
            return wup.at[0, :, cols]
        return wdown.at[0, cols, :]

    def fetch(kind, j, slot):
        pltpu.make_async_copy(src(kind, j), ring.at[slot], wsem.at[slot]).start()

    def arrived(slot):
        pltpu.make_async_copy(wout.at[0], ring.at[slot], wsem.at[slot]).wait()

    def put(idx, p, buf, out):
        return pltpu.make_async_copy(buf, out.at[pl.ds(pl.multiple_of(p * ROWS, ROWS), ROWS)], osem.at[idx, p])

    def fwd_copy(p):
        return pltpu.make_async_remote_copy(src_ref=hs.at[p], dst_ref=hin.at[p], send_sem=fs.at[p], recv_sem=fr.at[p],
                                            device_id=(data, right), device_id_type=MESH)

    def bwd_copy(p):
        return pltpu.make_async_remote_copy(src_ref=dhs.at[p], dst_ref=dho.at[p], send_sem=bs.at[p], recv_sem=br.at[p],
                                            device_id=(data, left), device_id_type=MESH)

    def loss_copy():
        return pltpu.make_async_remote_copy(src_ref=loss_in, dst_ref=loss_in, send_sem=ls.at[0], recv_sem=lr.at[0],
                                            device_id=(data, left), device_id_type=MESH)

    fetch('q', 0, 0)
    fetch('q', 1, 1)
    fetch('q', 2, 2)
    fetch('o', 0, 3)

    @pl.when(me == 0)
    def _():
        for p in range(2):
            pltpu.make_async_copy(x_ref.at[0, pl.ds(p * ROWS, ROWS)], hin.at[p], xsem.at[p]).start()

    @pl.when(me == last)
    def _():
        for p in range(2):
            pltpu.make_async_copy(y_ref.at[0, pl.ds(p * ROWS, ROWS)], dho.at[p], xsem.at[p]).start()

    barrier = pltpu.get_barrier_semaphore()
    for nb in (left, right):
        pl.semaphore_signal(barrier, inc=1, device_id=(data, nb), device_id_type=MESH)
    pl.semaphore_wait(barrier, 2)

    dgain_ref[...] = jnp.zeros_like(dgain_ref)

    @pl.when(me == last)
    def _():
        loss_in[...] = jnp.zeros_like(loss_in)
    qkv[pl.ds(ROWS, ROWS), pl.ds(D, 2 * D)] = jnp.zeros((ROWS, 2 * D), BF)
    gain0 = gain_ref[0, 0:1, :].astype(F32)
    gain1 = gain_ref[0, 1:2, :].astype(F32)
    low = lax.broadcasted_iota(jnp.int32, (ROWS, 2 * HEAD_DIM), 1) < HEAD_DIM

    def set_bias(p):
        r = lax.broadcasted_iota(jnp.int32, (ROWS, seq), 0) + p * ROWS
        c = lax.broadcasted_iota(jnp.int32, (ROWS, seq), 1)
        bias[...] = jnp.where(c <= r, 0.0, -1e30)

    def probs(qh, k):
        s = dot_nt(qh, k) * (HEAD_DIM ** -0.5 * LOG2E) + bias[...]
        e = jnp.exp2(s - jnp.max(s, axis=-1, keepdims=True))
        return e * (1.0 / jnp.sum(e, axis=-1, keepdims=True))

    def fwd_piece(p, carry):
        row0 = pl.multiple_of(p * ROWS, ROWS)
        rows = pl.ds(row0, ROWS)
        set_bias(p)

        @pl.when(me == 0)
        def _():
            pltpu.make_async_copy(x_ref.at[0, rows], hin.at[p], xsem.at[p]).wait()

        @pl.when(me > 0)
        def _():
            fwd_copy(p).wait_recv()

        h, inv = norm_stats(hin[p])
        n1[p] = (h * inv * gain0).astype(BF)
        put(0, p, n1.at[p], n1_o).start()

        @pl.loop(0, 3)
        def _(c):
            arrived(c)
            cols = pl.ds(pl.multiple_of(c * CH, CH), CH)
            qkv[rows, cols] = dot_nn(n1[p], ring[c]).astype(BF)

            @pl.when(c == 0)
            def _():
                fetch('u', 0, 0)

            @pl.when(c == 1)
            def _():
                fetch('d', 0, 1)

            @pl.when(c == 2)
            def _():
                fetch('u', 1, 2)

        @pl.loop(0, pairs)
        def _(i):
            co = pl.multiple_of(i * 2 * HEAD_DIM, 2 * HEAD_DIM)
            q = qkv[rows, pl.ds(co, 2 * HEAD_DIM)]
            k = qkv[:, pl.ds(D + co, 2 * HEAD_DIM)]
            v = qkv[:, pl.ds(2 * D + co, 2 * HEAD_DIM)]
            zero = jnp.zeros_like(q)
            outs = []
            for qh in (jnp.where(low, q, zero), jnp.where(low, zero, q)):
                outs.append(dot_nn(probs(qh, k).astype(BF), v))
            att[p, :, pl.ds(co, 2 * HEAD_DIM)] = jnp.where(low, outs[0], outs[1]).astype(BF)

        put(1, p, att.at[p], a_o).start()
        arrived(3)
        hmid[p] = (hin[p].astype(F32) + dot_nn(att[p], ring[3])).astype(BF)
        fetch('d', 1, 3)
        h, inv = norm_stats(hmid[p])
        n2[p] = (h * inv * gain1).astype(BF)
        put(2, p, n2.at[p], n2_o).start()
        acc[...] = hmid[p].astype(F32)

        @pl.loop(0, ffn_chunks)
        def _(j):
            cols = pl.ds(pl.multiple_of(j * CH, CH), CH)
            s0 = lax.rem(2 * j, 4)
            arrived(s0)
            u = dot_nn(n2[p], ring[s0])
            u_buf[rows, cols] = u

            @pl.when(j < 2)
            def _():
                fetch('u', j + 2, s0)

            @pl.when((j >= 2) & (p == 0))
            def _():
                fetch('q', (j - 2) * 2, s0)

            @pl.when((j >= 2) & (p == 1))
            def _():
                fetch('d', j - 2, s0)
            u2, t = gelu_parts(u_buf[rows, cols])
            act[p, :, cols] = (0.5 * u_buf[rows, cols] * (1.0 + t)).astype(BF)
            s1 = s0 + 1
            arrived(s1)
            acc[...] += dot_nn(act[p, :, cols], ring[s1])

            @pl.when(j < 2)
            def _():
                fetch('d', j + 2, s1)

            @pl.when((j == 2) & (p == 0))
            def _():
                fetch('q', 1, s1)

            @pl.when((j == 3) & (p == 0))
            def _():
                fetch('o', 0, s1)

            @pl.when((j >= 2) & (p == 1))
            def _():
                fetch('u', j - 2, s1)

        hs[p] = acc[...].astype(BF)

        @pl.when(me < last)
        def _():
            fwd_copy(p).start()

        put(3, p, act.at[p], act_o).start()

        @pl.when(me == last)
        def _():
            pltpu.make_async_copy(y_ref.at[0, rows], dho.at[p], xsem.at[p]).wait()
            err = hs[p].astype(F32) - dho[p].astype(F32)
            dho[p] = (err / count).astype(BF)
            part = jnp.sum(jnp.sum(err * err, axis=0, keepdims=True), axis=1, keepdims=True)
            loss_in[...] += part * (0.5 / count)
        return carry

    lax.fori_loop(0, 2, fwd_piece, 0)

    def bwd_piece(t, carry):
        p = 1 - t
        row0 = pl.multiple_of(p * ROWS, ROWS)
        rows = pl.ds(row0, ROWS)
        set_bias(p)

        @pl.when(me < last)
        def _():
            bwd_copy(p).wait_recv()

        @pl.when((me < last) & (t == 0))
        def _():
            loss_copy().wait_recv()

        @pl.when((me > 0) & (t == 0))
        def _():
            loss_copy().start()
        put(7, p, dho.at[p], dho_o).start()
        acc[...] = jnp.zeros_like(acc)

        @pl.loop(0, ffn_chunks)
        def _(j):
            cols = pl.ds(pl.multiple_of(j * CH, CH), CH)
            s0 = lax.rem(2 * j, 4)
            arrived(s0)
            dact = dot_nt(dho[p], ring[s0])

            @pl.when(j < 2)
            def _():
                fetch('d', j + 2, s0)

            @pl.when(j == 2)
            def _():
                fetch('o', 0, s0)

            @pl.when(j == 3)
            def _():
                fetch('q', 1, s0)
            u = u_buf[rows, cols]
            u2, th = gelu_parts(u)
            slope = 0.5 * (1.0 + th) + (0.5 * u) * (1.0 - th * th) * (GELU_C + (3.0 * GELU_C * GELU_A) * u2)
            du[p, :, cols] = (dact * slope).astype(BF)
            s1 = s0 + 1
            arrived(s1)
            acc[...] += dot_nt(du[p, :, cols], ring[s1])

            @pl.when(j < 2)
            def _():
                fetch('u', j + 2, s1)

            @pl.when(j == 2)
            def _():
                fetch('q', 0, s1)

            @pl.when(j == 3)
            def _():
                fetch('q', 2, s1)

        put(4, p, du.at[p], du_o).start()
        dh, dg = norm_grad(acc[...], hmid[p], gain1)
        dgain_ref[1:2, :] += dg
        dhm[p] = (dho[p].astype(F32) + dh).astype(BF)
        put(6, p, dhm.at[p], dhm_o).start()
        arrived(0)
        da[...] = dot_nt(dhm[p], ring[0]).astype(BF)

        @pl.when(t == 0)
        def _():
            fetch('d', 0, 0)

        @pl.loop(0, pairs)
        def _(i):
            co = pl.multiple_of(i * 2 * HEAD_DIM, 2 * HEAD_DIM)
            lanes = pl.ds(co, 2 * HEAD_DIM)
            q = qkv[rows, lanes]
            k = qkv[:, pl.ds(D + co, 2 * HEAD_DIM)]
            v = qkv[:, pl.ds(2 * D + co, 2 * HEAD_DIM)]
            do = da[:, lanes]
            prod = do.astype(F32) * att[p, :, lanes].astype(F32)
            zero = jnp.zeros_like(q)
            dqs = []
            dk = jnp.zeros((seq, 2 * HEAD_DIM), F32)
            dv = jnp.zeros((seq, 2 * HEAD_DIM), F32)
            for hh in range(2):
                sel = low if hh == 0 else jnp.logical_not(low)
                qh = jnp.where(sel, q, zero)
                doh = jnp.where(sel, do, zero)
                pr = probs(qh, k)
                dp = dot_nt(doh, v)
                delta = jnp.sum(jnp.where(sel, prod, 0.0), axis=-1, keepdims=True)
                ds = (pr * (dp - delta) * (HEAD_DIM ** -0.5)).astype(BF)
                dqs.append(dot_nn(ds, k))
                dk = dk + dot_tn(ds, qh)
                dv = dv + dot_tn(pr.astype(BF), doh)
            dqkv[p, :, lanes] = jnp.where(low, dqs[0], dqs[1]).astype(BF)
            klanes = pl.ds(D + co, 2 * HEAD_DIM)
            vlanes = pl.ds(2 * D + co, 2 * HEAD_DIM)

            @pl.when(t == 0)
            def _():
                dqkv[p, :, klanes] = dk[ROWS:].astype(BF)
                dqkv[p, :, vlanes] = dv[ROWS:].astype(BF)
                dkv[:, lanes] = dk[:ROWS]
                dkv[:, klanes] = dv[:ROWS]

            @pl.when(t == 1)
            def _():
                dqkv[p, :, klanes] = (dk[:ROWS] + dkv[:, lanes]).astype(BF)
                dqkv[p, :, vlanes] = (dv[:ROWS] + dkv[:, klanes]).astype(BF)

        put(5, p, dqkv.at[p], dqkv_o).start()
        acc[...] = jnp.zeros_like(acc)

        @pl.loop(0, 3)
        def _(c):
            arrived(c + 1)
            cols = pl.ds(pl.multiple_of(c * CH, CH), CH)
            acc[...] += dot_nt(dqkv[p, :, cols], ring[c + 1])

            @pl.when((c == 0) & (t == 0))
            def _():
                fetch('u', 0, 1)

            @pl.when((c == 1) & (t == 0))
            def _():
                fetch('d', 1, 2)

            @pl.when((c == 2) & (t == 0))
            def _():
                fetch('u', 1, 3)

        dh, dg = norm_grad(acc[...], hin[p], gain0)
        dgain_ref[0:1, :] += dg

        @pl.when(me > 0)
        def _():
            dhs[p] = (dhm[p].astype(F32) + dh).astype(BF)
            bwd_copy(p).start()
        return carry

    lax.fori_loop(0, 2, bwd_piece, 0)
    loss_ref[...] = loss_in[...]

    for p in range(2):
        for idx, (buf, out) in enumerate(((n1, n1_o), (att, a_o), (n2, n2_o), (act, act_o), (du, du_o), (dqkv, dqkv_o), (dhm, dhm_o), (dho, dho_o))):
            put(idx, p, buf.at[p], out).wait()

        @pl.when(me < last)
        def _():
            fwd_copy(p).wait_send()

        @pl.when(me > 0)
        def _():
            bwd_copy(p).wait_send()

    @pl.when(me > 0)
    def _():
        loss_copy().wait_send()


def run_pipeline(stages, x, y, w_qkv, w_out, w_up, w_down, gain):
    seq, width = x.shape[1], x.shape[2]
    ffn = w_up.shape[2]
    hbm = pl.BlockSpec(memory_space=pl.ANY)
    vmem = pl.BlockSpec(memory_space=pltpu.VMEM)
    V = pltpu.VMEM
    piece = (2, ROWS, width)
    widths = (width, width, width, ffn, ffn, 3 * width, width, width)
    outs = [jax.ShapeDtypeStruct((8, 128), F32), jax.ShapeDtypeStruct((2, width), F32)]
    outs += [jax.ShapeDtypeStruct((seq, w), BF) for w in widths]
    dma = pltpu.SemaphoreType.DMA
    return pl.pallas_call(
        functools.partial(pipeline_kernel, stages, seq, width),
        out_shape=outs,
        in_specs=[hbm] * 6 + [vmem],
        out_specs=[vmem, vmem] + [hbm] * 8,
        scratch_shapes=[
            V((4, width, width), BF),
            V(piece, BF), V(piece, BF), V(piece, BF),
            V(piece, BF), V(piece, BF), V(piece, BF),
            V((seq, 3 * width), BF),
            V((seq, ffn), F32),
            V((2, ROWS, ffn), BF),
            V((ROWS, width), F32),
            V(piece, BF), V(piece, BF), V(piece, BF), V((ROWS, width), BF),
            V((2, ROWS, ffn), BF), V((2, ROWS, 3 * width), BF),
            V((ROWS, 2 * width), F32),
            V((ROWS, seq), F32), V((8, 128), F32),
            dma((4,)), dma((2,)), dma((8, 2)),
            dma((2,)), dma((2,)), dma((2,)), dma((2,)), dma((1,)), dma((1,)),
        ],
        compiler_params=pltpu.CompilerParams(collective_id=0, has_side_effects=True, vmem_limit_bytes=67043328),
        name='pipeline',
    )(x, y, w_qkv, w_out, w_up, w_down, gain)


def solution(mesh):
    stages = mesh.shape['stage']

    def per_device(x, y, w_qkv, w_out, w_up, w_down, norm_gain):
        loss, dgain, n1, att, n2, act, du, dqkv, dhm, dho = run_pipeline(stages, x, y, w_qkv, w_out, w_up, w_down, norm_gain)
        g_qkv = dot_tn(n1, dqkv)
        g_out = dot_tn(att, dhm)
        g_up = dot_tn(n2, du)
        g_down = dot_tn(act, dho)
        return loss[0, 0].reshape(1), g_qkv[None], g_out[None], g_up[None], g_down[None], dgain[None]

    weight_spec = P('stage')
    grad_spec = P(('data', 'stage'))
    return jax.shard_map(per_device, mesh=mesh, in_specs=(P('data'), P('data')) + (weight_spec,) * 5,
                         out_specs=(P('data'),) + (grad_spec,) * 5, check_vma=False)
```

```python
import functools
import math

import jax
import jax.numpy as jnp
from jax import lax
from jax.experimental import pallas as pl
from jax.experimental.pallas import tpu as pltpu
from jax.sharding import PartitionSpec as P

MESH = pl.DeviceIdType.MESH
BF = jnp.bfloat16
F32 = jnp.float32
HEAD_DIM = 64
ROWS = 128
RING = 6
CHUNKS = 12
EPS = 1e-6
GELU_C = math.sqrt(2.0 / math.pi)
GELU_A = 0.044715
LOG2E = math.log2(math.e)


def dot_nn(a, b):
    return jnp.dot(a, b, preferred_element_type=F32)


def dot_nt(a, b):
    return lax.dot_general(a, b, (((1,), (1,)), ((), ())), preferred_element_type=F32)


def dot_tn(a, b):
    return lax.dot_general(a, b, (((0,), (0,)), ((), ())), preferred_element_type=F32)


def norm_stats(h_bf):
    h = h_bf.astype(F32)
    inv = lax.rsqrt(jnp.mean(h * h, axis=-1, keepdims=True) + EPS)
    return h, inv


def norm_grad(dn, h_bf, gain):
    h, inv = norm_stats(h_bf)
    hhat = h * inv
    dgain = jnp.sum(dn * hhat, axis=0, keepdims=True)
    dhhat = dn * gain
    corr = jnp.mean(dhhat * hhat, axis=-1, keepdims=True)
    return inv * (dhhat - hhat * corr), dgain


def gelu_parts(u):
    u2 = u * u
    t = jnp.tanh(u * (GELU_C + (GELU_C * GELU_A) * u2))
    return u2, t


def pipeline_kernel(stages, seq, width, x_ref, y_ref, wqkv, wout, wup, wdown, gain_ref,
                    loss_ref, dgain_ref, n1_o, a_o, n2_o, act_o, du_o, dqkv_o, dhm_o, dho_o, wt,
                    ring, hin, hs, hmid, n1, att, n2, qkv, u_buf, act, acc, dho, dhs, dhm, da, du, dqkv, dkvt, bias, loss_in,
                    sb0, sb1, tb0, tb1, pb0, pb1, gb0, gb1,
                    wsem, tsem, xsem, osem, fs, fr, bs, br, ls, lr):
    me = lax.axis_index('stage')
    data = lax.axis_index('data')
    last = stages - 1
    half = stages // 2
    right = lax.rem(me + 1, stages)
    left = lax.rem(me + stages - 1, stages)
    D = width
    CH = D
    LN = 2 * HEAD_DIM
    pairs = D // LN
    pieces = seq // ROWS
    count = float(seq * width)
    sbuf, tbuf, pbuf, gbuf = (sb0, sb1), (tb0, tb1), (pb0, pb1), (gb0, gb1)

    def fetch(kind, j, slot):
        cols = pl.ds(pl.multiple_of(j * CH, CH), CH)
        src = {'q': lambda: wqkv.at[0, :, cols], 'o': lambda: wout.at[0], 'u': lambda: wup.at[0, :, cols], 'd': lambda: wdown.at[0, cols, :]}[kind]()
        pltpu.make_async_copy(src, ring.at[slot], wsem.at[slot]).start()

    def fetch_bwd(idx):
        slot = lax.rem(idx, RING)
        pltpu.make_async_copy(wt.at[idx], ring.at[slot], wsem.at[slot]).start()

    def arrived(slot):
        pltpu.make_async_copy(wout.at[0], ring.at[slot], wsem.at[slot]).wait()

    def put(idx, p, buf, out):
        return pltpu.make_async_copy(buf, out.at[pl.ds(pl.multiple_of(p * ROWS, ROWS), ROWS)], osem.at[idx, p])

    def fwd_copy(p):
        return pltpu.make_async_remote_copy(src_ref=hs.at[p], dst_ref=hin.at[p], send_sem=fs.at[p], recv_sem=fr.at[p],
                                            device_id=(data, right), device_id_type=MESH)

    def bwd_copy(p):
        return pltpu.make_async_remote_copy(src_ref=dhs.at[p], dst_ref=dho.at[p], send_sem=bs.at[p], recv_sem=br.at[p],
                                            device_id=(data, left), device_id_type=MESH)

    def loss_copy():
        return pltpu.make_async_remote_copy(src_ref=loss_in, dst_ref=loss_in, send_sem=ls.at[0], recv_sem=lr.at[0],
                                            device_id=(data, left), device_id_type=MESH)

    def transpose_weights():
        def fetch_any(b):
            slot = lax.rem(b, 3)
            for odd, kind in ((0, 'd'), (1, 'u')):
                @pl.when((b < 8) & (lax.rem(b, 2) == odd))
                def _(kind=kind):
                    fetch(kind, lax.div(b, 2), slot)

            @pl.when(b == 8)
            def _():
                fetch('o', 0, slot)

            @pl.when(b > 8)
            def _():
                fetch('q', b - 9, slot)

        def store(b):
            slot = lax.rem(b, 3)
            return pltpu.make_async_copy(ring.at[slot + 3], wt.at[b], tsem.at[slot])

        fetch_any(0)
        fetch_any(1)

        @pl.loop(0, CHUNKS)
        def _(b):
            slot = lax.rem(b, 3)

            @pl.when(b + 2 < CHUNKS)
            def _():
                fetch_any(b + 2)
            arrived(slot)

            @pl.when(b >= 3)
            def _():
                store(b - 3).wait()

            @pl.loop(0, D // 256)
            def _(r):
                blk = pl.ds(pl.multiple_of(r * 256, 256), 256)
                ring[slot + 3, :, blk] = ring[slot, blk, :].T
            store(b).start()

        @pl.loop(CHUNKS - 3, CHUNKS)
        def _(b):
            store(b).wait()

    def start_fwd():
        for c in range(3):
            fetch('q', c, c)
        fetch('o', 0, 3)
        fetch('u', 0, 4)
        fetch('d', 0, 5)

    @pl.when(me < half)
    def _():
        start_fwd()

    @pl.when(me == 0)
    def _():
        for p in range(pieces):
            pltpu.make_async_copy(x_ref.at[0, pl.ds(p * ROWS, ROWS)], hin.at[p], xsem.at[p]).start()

    @pl.when(me == last)
    def _():
        for p in range(pieces):
            pltpu.make_async_copy(y_ref.at[0, pl.ds(p * ROWS, ROWS)], dho.at[p], xsem.at[p]).start()

    barrier = pltpu.get_barrier_semaphore()
    for nb in (left, right):
        pl.semaphore_signal(barrier, inc=1, device_id=(data, nb), device_id_type=MESH)
    pl.semaphore_wait(barrier, 2)

    @pl.when(me >= half)
    def _():
        transpose_weights()
        start_fwd()

    dgain_ref[...] = jnp.zeros_like(dgain_ref)

    @pl.when(me == last)
    def _():
        loss_in[...] = jnp.zeros_like(loss_in)
    qkv[pl.ds(ROWS, seq - ROWS), pl.ds(D, 2 * D)] = jnp.zeros((seq - ROWS, 2 * D), BF)
    gain0 = gain_ref[0, 0:1, :].astype(F32)
    gain1 = gain_ref[0, 1:2, :].astype(F32)
    low = lax.broadcasted_iota(jnp.int32, (ROWS, LN), 1) < HEAD_DIM

    def stack(a):
        zero = jnp.zeros_like(a)
        return jnp.concatenate([jnp.where(low, a, zero), jnp.where(low, zero, a)], axis=0)

    def unstack(a):
        return jnp.where(low, a[:ROWS], a[ROWS:])

    def lanes(i, base=0):
        return pl.ds(pl.multiple_of(i * LN, LN) + base, LN)

    def set_bias(p):
        r = lax.rem(lax.broadcasted_iota(jnp.int32, (2 * ROWS, seq), 0), ROWS) + p * ROWS
        c = lax.broadcasted_iota(jnp.int32, (2 * ROWS, seq), 1)
        bias[...] = jnp.where(c <= r, 0.0, -1e30)

    def probs(s):
        s = s * (HEAD_DIM ** -0.5 * LOG2E) + bias[...]
        e = jnp.exp2(s - jnp.max(s, axis=-1, keepdims=True))
        return e * (1.0 / jnp.sum(e, axis=-1, keepdims=True))

    def pair_pipeline(first, middle, final):
        first(0, 0)

        @pl.loop(0, pairs // 2)
        def _(h):
            i = 2 * h
            first(i + 1, 1)
            middle(i, 0)
            final(jnp.maximum(i - 1, 0), 1)
            first(jnp.minimum(i + 2, pairs - 1), 0)
            middle(i + 1, 1)
            final(i, 0)
        final(pairs - 1, 1)

    def fwd_piece(p, carry):
        row0 = pl.multiple_of(p * ROWS, ROWS)
        rows = pl.ds(row0, ROWS)
        w = lax.rem(p, 2)
        set_bias(p)

        @pl.when(p >= 2)
        def _():
            put(0, p - 2, n1.at[w], n1_o).wait()
            put(2, p - 2, n2.at[w], n2_o).wait()
            put(3, p - 2, act.at[w], act_o).wait()

        @pl.when(me == 0)
        def _():
            pltpu.make_async_copy(x_ref.at[0, rows], hin.at[p], xsem.at[p]).wait()

        @pl.when(me > 0)
        def _():
            fwd_copy(p).wait_recv()

        def fetch_next(idx, kind, j):
            @pl.when(p < pieces - 1)
            def _():
                fetch(kind, j, idx)

            @pl.when((p == pieces - 1) & (me >= half))
            def _():
                fetch_bwd(idx)

        h, inv = norm_stats(hin[p])
        n1[w] = (h * inv * gain0).astype(BF)
        put(0, p, n1.at[w], n1_o).start()

        @pl.loop(0, 3)
        def _(c):
            arrived(c)
            cols = pl.ds(pl.multiple_of(c * CH, CH), CH)
            qkv[rows, cols] = dot_nn(n1[w], ring[c]).astype(BF)

            @pl.when(c == 0)
            def _():
                fetch('u', 1, 0)

            @pl.when(c == 1)
            def _():
                fetch('d', 1, 1)

            @pl.when(c == 2)
            def _():
                fetch('u', 2, 2)

        def scores(i, b):
            sbuf[b][...] = dot_nt(stack(qkv[rows, lanes(i)]), qkv[:, lanes(i, D)])

        def softmax(i, b):
            pbuf[b][...] = probs(sbuf[b][...]).astype(BF)

        def mix(i, b):
            att[p, :, lanes(i)] = unstack(dot_nn(pbuf[b][...], qkv[:, lanes(i, 2 * D)])).astype(BF)

        pair_pipeline(scores, softmax, mix)

        put(1, p, att.at[p], a_o).start()
        arrived(3)
        hmid[p] = (hin[p].astype(F32) + dot_nn(att[p], ring[3])).astype(BF)
        fetch('d', 2, 3)
        h, inv = norm_stats(hmid[p])
        n2[w] = (h * inv * gain1).astype(BF)
        put(2, p, n2.at[w], n2_o).start()
        acc[...] = hmid[p].astype(F32)

        @pl.loop(0, 4)
        def _(j):
            cols = pl.ds(pl.multiple_of(j * CH, CH), CH)
            s0 = lax.rem(2 * j + 4, RING)
            s1 = s0 + 1
            arrived(s0)
            u_buf[rows, cols] = dot_nn(n2[w], ring[s0])

            @pl.when(j == 0)
            def _():
                fetch('u', 3, 4)

            for jj, kind, jn in ((1, 'q', 0), (2, 'q', 2), (3, 'u', 0)):
                @pl.when(j == jj)
                def _(jj=jj, kind=kind, jn=jn):
                    fetch_next(2 * (jj - 1), kind, jn)
            u = u_buf[rows, cols]
            u2, t = gelu_parts(u)
            act[w, :, cols] = (0.5 * u * (1.0 + t)).astype(BF)
            arrived(s1)
            acc[...] += dot_nn(act[w, :, cols], ring[s1])

            @pl.when(j == 0)
            def _():
                fetch('d', 3, 5)

            for jj, kind, jn in ((1, 'q', 1), (2, 'o', 0), (3, 'd', 0)):
                @pl.when(j == jj)
                def _(jj=jj, kind=kind, jn=jn):
                    fetch_next(2 * (jj - 1) + 1, kind, jn)

        hs[p] = acc[...].astype(BF)

        @pl.when(me < last)
        def _():
            fwd_copy(p).start()

        put(3, p, act.at[w], act_o).start()

        @pl.when(me == last)
        def _():
            pltpu.make_async_copy(y_ref.at[0, rows], dho.at[p], xsem.at[p]).wait()
            err = hs[p].astype(F32) - dho[p].astype(F32)
            dho[p] = (err / count).astype(BF)
            part = jnp.sum(jnp.sum(err * err, axis=0, keepdims=True), axis=1, keepdims=True)
            loss_in[...] += part * (0.5 / count)
        return carry

    lax.fori_loop(0, pieces, fwd_piece, 0)

    @pl.when(me < half)
    def _():
        transpose_weights()
        for b in range(RING):
            fetch_bwd(b)
    dkvt[...] = jnp.zeros_like(dkvt)

    def bwd_piece(t, carry):
        p = pieces - 1 - t
        row0 = pl.multiple_of(p * ROWS, ROWS)
        rows = pl.ds(row0, ROWS)
        w = lax.rem(t, 2)
        set_bias(p)
        for b in range(2):
            pbuf[b][...] = jnp.zeros_like(pbuf[b])
            gbuf[b][...] = jnp.zeros_like(gbuf[b])

        @pl.when(t >= 2)
        def _():
            put(4, p + 2, du.at[w], du_o).wait()
            put(5, p + 2, dqkv.at[w], dqkv_o).wait()
            put(6, p + 2, dhm.at[w], dhm_o).wait()

        @pl.when(me < last)
        def _():
            bwd_copy(p).wait_recv()

        @pl.when((me < last) & (t == 0))
        def _():
            loss_copy().wait_recv()

        @pl.when((me > 0) & (t == 0))
        def _():
            loss_copy().start()
        put(7, p, dho.at[p], dho_o).start()

        def fetch_next(idx):
            nxt = idx + RING

            @pl.when(nxt < CHUNKS)
            def _():
                fetch_bwd(nxt)

            @pl.when((nxt >= CHUNKS) & (t < pieces - 1))
            def _():
                fetch_bwd(nxt - CHUNKS)

        acc[...] = jnp.zeros_like(acc)

        @pl.loop(0, 4)
        def _(j):
            cols = pl.ds(pl.multiple_of(j * CH, CH), CH)
            s0 = lax.rem(2 * j, RING)
            s1 = s0 + 1
            arrived(s0)
            dact = dot_nn(dho[p], ring[s0])
            u = u_buf[rows, cols]
            u2, th = gelu_parts(u)
            slope = 0.5 * (1.0 + th) + (0.5 * u) * (1.0 - th * th) * (GELU_C + (3.0 * GELU_C * GELU_A) * u2)
            du[w, :, cols] = (dact * slope).astype(BF)
            fetch_next(2 * j)
            arrived(s1)
            acc[...] += dot_nn(du[w, :, cols], ring[s1])
            fetch_next(2 * j + 1)

        put(4, p, du.at[w], du_o).start()
        dh, dg = norm_grad(acc[...], hmid[p], gain1)
        dgain_ref[1:2, :] += dg
        dhm[w] = (dho[p].astype(F32) + dh).astype(BF)
        put(6, p, dhm.at[w], dhm_o).start()
        arrived(8 % RING)
        da[...] = dot_nn(dhm[w], ring[8 % RING]).astype(BF)
        fetch_next(8)

        def scores(i, b):
            sbuf[b][...] = dot_nt(stack(qkv[rows, lanes(i)]), qkv[:, lanes(i, D)])
            tbuf[b][...] = dot_nt(stack(da[:, lanes(i)]), qkv[:, lanes(i, 2 * D)])

        def slopes(i, b):
            pr = probs(sbuf[b][...])
            prod = da[:, lanes(i)].astype(F32) * att[p, :, lanes(i)].astype(F32)
            both = jnp.concatenate([jnp.where(low, prod, 0.0), jnp.where(low, 0.0, prod)], axis=0)
            delta = jnp.sum(both, axis=-1, keepdims=True)
            pbuf[b][...] = pr.astype(BF)
            gbuf[b][...] = (pr * (tbuf[b][...] - delta)).astype(BF)

        def grads(i, b):
            scale = HEAD_DIM ** -0.5
            dqkv[w, :, lanes(i)] = (unstack(dot_nn(gbuf[b][...], qkv[:, lanes(i, D)])) * scale).astype(BF)
            dkvt[lanes(i), :] += dot_tn(stack(qkv[rows, lanes(i)]) * scale, gbuf[b][...])
            dkvt[lanes(i, D), :] += dot_tn(stack(da[:, lanes(i)]), pbuf[b][...])

        pair_pipeline(scores, slopes, grads)

        @pl.loop(0, 2 * pairs)
        def _(i):
            dqkv[w, :, lanes(i, D)] = dkvt[lanes(i), rows].T.astype(BF)

        put(5, p, dqkv.at[w], dqkv_o).start()
        acc[...] = jnp.zeros_like(acc)

        @pl.loop(0, 3)
        def _(c):
            slot = c + 9 % RING
            arrived(slot)
            cols = pl.ds(pl.multiple_of(c * CH, CH), CH)
            acc[...] += dot_nn(dqkv[w, :, cols], ring[slot])
            fetch_next(c + 9)

        dh, dg = norm_grad(acc[...], hin[p], gain0)
        dgain_ref[0:1, :] += dg

        @pl.when(me > 0)
        def _():
            dhs[p] = (dhm[w].astype(F32) + dh).astype(BF)
            bwd_copy(p).start()
        return carry

    lax.fori_loop(0, pieces, bwd_piece, 0)
    loss_ref[...] = loss_in[...]

    for p in range(pieces):
        put(1, p, att.at[p], a_o).wait()
        put(7, p, dho.at[p], dho_o).wait()

        @pl.when(me < last)
        def _():
            fwd_copy(p).wait_send()

        @pl.when(me > 0)
        def _():
            bwd_copy(p).wait_send()
    for e in range(2):
        p = pieces - 2 + e
        put(0, p, n1.at[e], n1_o).wait()
        put(2, p, n2.at[e], n2_o).wait()
        put(3, p, act.at[e], act_o).wait()
        put(4, e, du.at[1 - e], du_o).wait()
        put(5, e, dqkv.at[1 - e], dqkv_o).wait()
        put(6, e, dhm.at[1 - e], dhm_o).wait()

    @pl.when(me > 0)
    def _():
        loss_copy().wait_send()


def run_pipeline(stages, x, y, w_qkv, w_out, w_up, w_down, gain):
    seq, width = x.shape[1], x.shape[2]
    ffn = w_up.shape[2]
    pieces = seq // ROWS
    hbm = pl.BlockSpec(memory_space=pl.ANY)
    vmem = pl.BlockSpec(memory_space=pltpu.VMEM)
    V = pltpu.VMEM
    full = V((pieces, ROWS, width), BF)
    two = V((2, ROWS, width), BF)
    wide = V((2 * ROWS, seq), F32)
    tight = V((2 * ROWS, seq), BF)
    widths = (width, width, width, ffn, ffn, 3 * width, width, width)
    outs = [jax.ShapeDtypeStruct((8, 128), F32), jax.ShapeDtypeStruct((2, width), F32)]
    outs += [jax.ShapeDtypeStruct((seq, w), BF) for w in widths]
    outs += [jax.ShapeDtypeStruct((CHUNKS, width, width), BF)]
    dma = pltpu.SemaphoreType.DMA
    return pl.pallas_call(
        functools.partial(pipeline_kernel, stages, seq, width),
        out_shape=outs,
        in_specs=[hbm] * 6 + [vmem],
        out_specs=[vmem, vmem] + [hbm] * 9,
        scratch_shapes=[
            V((RING, width, width), BF),
            full, full, full,
            two, full, two,
            V((seq, 3 * width), BF),
            V((seq, ffn), F32),
            V((2, ROWS, ffn), BF),
            V((ROWS, width), F32),
            full, full, two, V((ROWS, width), BF),
            V((2, ROWS, ffn), BF), V((2, ROWS, 3 * width), BF),
            V((2 * width, seq), F32),
            wide, V((8, 128), F32),
            wide, wide, wide, wide, tight, tight, tight, tight,
            dma((RING,)), dma((3,)), dma((pieces,)), dma((8, pieces)),
            dma((pieces,)), dma((pieces,)), dma((pieces,)), dma((pieces,)), dma((1,)), dma((1,)),
        ],
        compiler_params=pltpu.CompilerParams(collective_id=0, has_side_effects=True, vmem_limit_bytes=67043328),
        name='pipeline',
    )(x, y, w_qkv, w_out, w_up, w_down, gain)


def solution(mesh):
    stages = mesh.shape['stage']

    def per_device(x, y, w_qkv, w_out, w_up, w_down, norm_gain):
        loss, dgain, n1, att, n2, act, du, dqkv, dhm, dho, _ = run_pipeline(stages, x, y, w_qkv, w_out, w_up, w_down, norm_gain)
        g_qkv = dot_tn(n1, dqkv)
        g_out = dot_tn(att, dhm)
        g_up = dot_tn(n2, du)
        g_down = dot_tn(act, dho)
        return loss[0, 0].reshape(1), g_qkv[None], g_out[None], g_up[None], g_down[None], dgain[None]

    weight_spec = P('stage')
    grad_spec = P(('data', 'stage'))
    return jax.shard_map(per_device, mesh=mesh, in_specs=(P('data'), P('data')) + (weight_spec,) * 5,
                         out_specs=(P('data'),) + (grad_spec,) * 5, check_vma=False)
```

```python
import functools
import math

import jax
import jax.numpy as jnp
from jax import lax
from jax.experimental import pallas as pl
from jax.experimental.pallas import tpu as pltpu
from jax.sharding import PartitionSpec as P

MESH = pl.DeviceIdType.MESH
BF = jnp.bfloat16
F32 = jnp.float32
HEAD_DIM = 64
ROWS = 128
RING = 6
CHUNKS = 12
STAGES = 3
EPS = 1e-6
GELU_C = math.sqrt(2.0 / math.pi)
GELU_A = 0.044715
LOG2E = math.log2(math.e)


def dot_nn(a, b):
    return jnp.dot(a, b, preferred_element_type=F32)


def dot_nt(a, b):
    return lax.dot_general(a, b, (((1,), (1,)), ((), ())), preferred_element_type=F32)


def dot_tn(a, b):
    return lax.dot_general(a, b, (((0,), (0,)), ((), ())), preferred_element_type=F32)


def norm_stats(h_bf):
    h = h_bf.astype(F32)
    inv = lax.rsqrt(jnp.mean(h * h, axis=-1, keepdims=True) + EPS)
    return h, inv


def norm_grad(dn, h_bf, gain):
    h, inv = norm_stats(h_bf)
    hhat = h * inv
    dgain = jnp.sum(dn * hhat, axis=0, keepdims=True)
    dhhat = dn * gain
    corr = jnp.mean(dhhat * hhat, axis=-1, keepdims=True)
    return inv * (dhhat - hhat * corr), dgain


def gelu_parts(u):
    u2 = u * u
    t = jnp.tanh(u * (GELU_C + (GELU_C * GELU_A) * u2))
    return u2, t


def pipeline_kernel(stages, seq, width, x_ref, y_ref, wqkv, wout, wup, wdown, gain_ref,
                    loss_ref, dgain_ref, n1_o, a_o, n2_o, act_o, du_o, dqkv_o, dhm_o, dho_o, wt,
                    ring, hin, hs, hmid, n1, att, n2, qkv, u_buf, act, acc, dho, bias, loss_in,
                    sb0, sb1, pb0, pb1,
                    wsem, esem, tsem, xsem, osem, fs, fr, bs, br, ls, lr):
    me = lax.axis_index('stage')
    data = lax.axis_index('data')
    last = stages - 1
    half = stages // 2
    right = lax.rem(me + 1, stages)
    left = lax.rem(me + stages - 1, stages)
    D = width
    CH = D
    LN = 2 * HEAD_DIM
    pairs = D // LN
    pieces = seq // ROWS
    count = float(seq * width)
    sbuf, pbuf = (sb0, sb1), (pb0, pb1)

    def fetch(kind, j, slot, extra=None):
        cols = pl.ds(pl.multiple_of(j * CH, CH), CH)
        src = {'q': lambda: wqkv.at[0, :, cols], 'o': lambda: wout.at[0], 'u': lambda: wup.at[0, :, cols], 'd': lambda: wdown.at[0, cols, :]}[kind]()
        if extra is None:
            pltpu.make_async_copy(src, ring.at[slot], wsem.at[slot]).start()
        else:
            pltpu.make_async_copy(src, extra.at[slot], esem.at[slot]).start()

    def fetch_bwd(idx):
        slot = lax.rem(idx, RING)
        pltpu.make_async_copy(wt.at[idx], ring.at[slot], wsem.at[slot]).start()

    def arrived(slot):
        pltpu.make_async_copy(wout.at[0], ring.at[slot], wsem.at[slot]).wait()

    def put(idx, p, buf, out):
        return pltpu.make_async_copy(buf, out.at[pl.ds(pl.multiple_of(p * ROWS, ROWS), ROWS)], osem.at[idx, p])

    def fwd_copy(p):
        return pltpu.make_async_remote_copy(src_ref=hs.at[p], dst_ref=hin.at[p], send_sem=fs.at[p], recv_sem=fr.at[p],
                                            device_id=(data, right), device_id_type=MESH)

    def bwd_copy(p):
        return pltpu.make_async_remote_copy(src_ref=hs.at[p], dst_ref=dho.at[p], send_sem=bs.at[p], recv_sem=br.at[p],
                                            device_id=(data, left), device_id_type=MESH)

    def loss_copy():
        return pltpu.make_async_remote_copy(src_ref=loss_in, dst_ref=loss_in, send_sem=ls.at[0], recv_sem=lr.at[0],
                                            device_id=(data, left), device_id_type=MESH)

    def transpose_weights():
        def fetch_any(b):
            slot = lax.rem(b, 3)
            for odd, kind in ((0, 'd'), (1, 'u')):
                @pl.when((b < 8) & (lax.rem(b, 2) == odd))
                def _(kind=kind):
                    fetch(kind, lax.div(b, 2), slot)

            @pl.when(b == 8)
            def _():
                fetch('o', 0, slot)

            @pl.when(b > 8)
            def _():
                fetch('q', b - 9, slot)

        def store(b):
            slot = lax.rem(b, 3)
            return pltpu.make_async_copy(ring.at[slot + 3], wt.at[b], tsem.at[slot])

        fetch_any(0)
        fetch_any(1)

        @pl.loop(0, CHUNKS)
        def _(b):
            slot = lax.rem(b, 3)

            @pl.when(b + 2 < CHUNKS)
            def _():
                fetch_any(b + 2)
            arrived(slot)

            @pl.when(b >= 3)
            def _():
                store(b - 3).wait()

            @pl.loop(0, D // 256)
            def _(r):
                blk = pl.ds(pl.multiple_of(r * 256, 256), 256)
                ring[slot + 3, :, blk] = ring[slot, blk, :].T
            store(b).start()

        @pl.loop(CHUNKS - 3, CHUNKS)
        def _(b):
            store(b).wait()

    def start_fwd(extra):
        for c in range(3):
            fetch('q', c, c)
        fetch('o', 0, 3)
        fetch('u', 0, 4)
        fetch('d', 0, 5)
        for e, (kind, j) in enumerate((('u', 1), ('d', 1), ('u', 2), ('d', 2), ('d', 3))):
            fetch(kind, j, e, extra)

    @pl.when(me == 0)
    def _():
        for p in range(pieces):
            pltpu.make_async_copy(x_ref.at[0, pl.ds(p * ROWS, ROWS)], hin.at[p], xsem.at[p]).start()

    @pl.when(me == last)
    def _():
        for p in range(pieces):
            pltpu.make_async_copy(y_ref.at[0, pl.ds(p * ROWS, ROWS)], dho.at[p], xsem.at[p]).start()

    barrier = pltpu.get_barrier_semaphore()
    for nb in (left, right):
        pl.semaphore_signal(barrier, inc=1, device_id=(data, nb), device_id_type=MESH)
    pl.semaphore_wait(barrier, 2)

    @pl.when(me >= half)
    def _():
        transpose_weights()

    dgain_ref[...] = jnp.zeros_like(dgain_ref)

    @pl.when(me == last)
    def _():
        loss_in[...] = jnp.zeros_like(loss_in)
    qkv[pl.ds(ROWS, seq - ROWS), pl.ds(D, 2 * D)] = jnp.zeros((seq - ROWS, 2 * D), BF)
    gain0 = gain_ref[0, 0:1, :].astype(F32)
    gain1 = gain_ref[0, 1:2, :].astype(F32)
    low = lax.broadcasted_iota(jnp.int32, (ROWS, LN), 1) < HEAD_DIM

    def stack(a):
        zero = jnp.zeros_like(a)
        return jnp.concatenate([jnp.where(low, a, zero), jnp.where(low, zero, a)], axis=0)

    def unstack(a):
        return jnp.where(low, a[:ROWS], a[ROWS:])

    def lanes(i, base=0):
        return pl.ds(pl.multiple_of(i * LN, LN) + base, LN)

    def set_bias(p):
        r = lax.rem(lax.broadcasted_iota(jnp.int32, (2 * ROWS, seq), 0), ROWS) + p * ROWS
        c = lax.broadcasted_iota(jnp.int32, (2 * ROWS, seq), 1)
        bias[...] = jnp.where(c <= r, 0.0, -1e30)

    def probs(s):
        s = s * (HEAD_DIM ** -0.5 * LOG2E) + bias[...]
        e = jnp.exp2(s - jnp.max(s, axis=-1, keepdims=True))
        return e * (1.0 / jnp.sum(e, axis=-1, keepdims=True))

    def pair_pipeline(first, middle, final):
        first(0, 0)

        @pl.loop(0, pairs // 2)
        def _(h):
            i = 2 * h
            first(i + 1, 1)
            middle(i, 0)
            final(jnp.maximum(i - 1, 0), 1)
            first(jnp.minimum(i + 2, pairs - 1), 0)
            middle(i + 1, 1)
            final(i, 0)
        final(pairs - 1, 1)

    def fwd_piece(extra, p, carry):
        row0 = pl.multiple_of(p * ROWS, ROWS)
        rows = pl.ds(row0, ROWS)
        w = lax.rem(p, 2)
        set_bias(p)

        @pl.when(p >= 2)
        def _():
            put(0, p - 2, n1.at[w], n1_o).wait()
            put(2, p - 2, n2.at[w], n2_o).wait()
            put(3, p - 2, act.at[w], act_o).wait()

        @pl.when(me == 0)
        def _():
            pltpu.make_async_copy(x_ref.at[0, rows], hin.at[p], xsem.at[p]).wait()

        @pl.when(me > 0)
        def _():
            fwd_copy(p).wait_recv()

        @pl.when(p == 0)
        def _():
            for c in range(3):
                arrived(c)

        turn = (p == pieces - 1) & (me >= half)

        h, inv = norm_stats(hin[p])
        n1[w] = (h * inv * gain0).astype(BF)
        put(0, p, n1.at[w], n1_o).start()

        for c in range(3):
            qkv[rows, c * CH:(c + 1) * CH] = dot_nn(n1[w], ring[c]).astype(BF)

        @pl.when(turn)
        def _():
            for c in range(3):
                fetch_bwd(c)

        def scores(i, b):
            sbuf[b][...] = dot_nt(stack(qkv[rows, lanes(i)]), qkv[:, lanes(i, D)])

        def softmax(i, b):
            pbuf[b][...] = probs(sbuf[b][...]).astype(BF)

        def mix(i, b):
            att[p, :, lanes(i)] = unstack(dot_nn(pbuf[b][...], qkv[:, lanes(i, 2 * D)])).astype(BF)

        pair_pipeline(scores, softmax, mix)

        put(1, p, att.at[p], a_o).start()
        arrived(3)
        hmid[p] = (hin[p].astype(F32) + dot_nn(att[p], ring[3])).astype(BF)
        fetch('u', 3, 3)
        h, inv = norm_stats(hmid[p])
        n2[w] = (h * inv * gain1).astype(BF)
        put(2, p, n2.at[w], n2_o).start()

        @pl.when(p == 0)
        def _():
            arrived(4)
            arrived(5)
            for e in range(5):
                pltpu.make_async_copy(wout.at[0], extra.at[e], esem.at[e]).wait()

        def up(j, weight):
            u_buf[rows, j * CH:(j + 1) * CH] = dot_nn(n2[w], weight[...])

        def down(j, weight):
            u = u_buf[rows, j * CH:(j + 1) * CH]
            u2, t = gelu_parts(u)
            act[w, :, j * CH:(j + 1) * CH] = (0.5 * u * (1.0 + t)).astype(BF)
            return dot_nn(act[w, :, j * CH:(j + 1) * CH], weight[...])

        up(0, ring.at[4])
        up(1, extra.at[0])
        acc[...] = hmid[p].astype(F32) + down(0, ring.at[5])
        up(2, extra.at[2])
        acc[...] += down(1, extra.at[1])
        arrived(3)
        up(3, ring.at[3])
        acc[...] += down(2, extra.at[3])
        hs[p] = (acc[...] + down(3, extra.at[4])).astype(BF)

        @pl.when(me < last)
        def _():
            fwd_copy(p).start()

        put(3, p, act.at[w], act_o).start()

        @pl.when(p < pieces - 1)
        def _():
            fetch('o', 0, 3)

        @pl.when(turn)
        def _():
            for b in range(3, RING):
                fetch_bwd(b)

        @pl.when(me == last)
        def _():
            pltpu.make_async_copy(y_ref.at[0, rows], dho.at[p], xsem.at[p]).wait()
            err = hs[p].astype(F32) - dho[p].astype(F32)
            dho[p] = (err / count).astype(BF)
            part = jnp.sum(jnp.sum(err * err, axis=0, keepdims=True), axis=1, keepdims=True)
            loss_in[...] += part * (0.5 / count)
        return carry

    def forward(extra):
        start_fwd(extra)
        lax.fori_loop(0, pieces, functools.partial(fwd_piece, extra), 0)

    pl.run_scoped(forward, pltpu.VMEM((5, D, D), BF))

    @pl.when(me < half)
    def _():
        transpose_weights()
        for b in range(RING):
            fetch_bwd(b)
    def bwd_piece(bufs, t, carry):
        tbuf, gbuf, dbuf, du, dqkv, dhm, da, dkvt = bufs
        p = pieces - 1 - t
        row0 = pl.multiple_of(p * ROWS, ROWS)
        rows = pl.ds(row0, ROWS)
        w = lax.rem(t, 2)
        set_bias(p)
        for b in range(2):
            pbuf[b][...] = jnp.zeros_like(pbuf[b])
            gbuf[b][...] = jnp.zeros_like(gbuf[b])

        @pl.when(t >= 2)
        def _():
            put(4, p + 2, du.at[w], du_o).wait()
            put(5, p + 2, dqkv.at[w], dqkv_o).wait()
            put(6, p + 2, dhm.at[w], dhm_o).wait()

        @pl.when(me < last)
        def _():
            bwd_copy(p).wait_recv()

        @pl.when((me < last) & (t == 0))
        def _():
            loss_copy().wait_recv()

        @pl.when((me > 0) & (t == 0))
        def _():
            loss_copy().start()
        put(7, p, dho.at[p], dho_o).start()

        def fetch_next(idx):
            nxt = idx + RING
            if nxt < CHUNKS:
                fetch_bwd(nxt)
            else:
                @pl.when(t < pieces - 1)
                def _():
                    fetch_bwd(nxt - CHUNKS)

        def back_down(j):
            arrived(2 * j % RING)
            dbuf[j % 2][...] = dot_nn(dho[p], ring[2 * j % RING])

        def back_up(j):
            cols = slice(j * CH, (j + 1) * CH)
            u = u_buf[rows, cols]
            u2, th = gelu_parts(u)
            slope = 0.5 * (1.0 + th) + (0.5 * u) * (1.0 - th * th) * (GELU_C + (3.0 * GELU_C * GELU_A) * u2)
            du[w, :, cols] = (dbuf[j % 2][...] * slope).astype(BF)
            return dot_nn(du[w, :, cols], ring[(2 * j + 1) % RING])

        back_down(0)
        fetch_next(0)
        for j in range(4):
            arrived((2 * j + 1) % RING)
            if j < 3:
                back_down(j + 1)
            part = back_up(j)
            if j == 0:
                acc[...] = part
            else:
                acc[...] += part
            fetch_next(2 * j + 1)
            if j < 3:
                fetch_next(2 * j + 2)

        put(4, p, du.at[w], du_o).start()
        dh, dg = norm_grad(acc[...], hmid[p], gain1)
        dgain_ref[1:2, :] += dg
        dhm[w] = (dho[p].astype(F32) + dh).astype(BF)
        put(6, p, dhm.at[w], dhm_o).start()
        arrived(8 % RING)
        da[...] = dot_nn(dhm[w], ring[8 % RING]).astype(BF)
        fetch_next(8)

        def scores(i, b):
            sbuf[b][...] = dot_nt(stack(qkv[rows, lanes(i)]), qkv[:, lanes(i, D)])
            tbuf[b][...] = dot_nt(stack(da[:, lanes(i)]), qkv[:, lanes(i, 2 * D)])

        def slopes(i, b):
            pr = probs(sbuf[b][...])
            prod = da[:, lanes(i)].astype(F32) * att[p, :, lanes(i)].astype(F32)
            both = jnp.concatenate([jnp.where(low, prod, 0.0), jnp.where(low, 0.0, prod)], axis=0)
            delta = jnp.sum(both, axis=-1, keepdims=True)
            pbuf[b][...] = pr.astype(BF)
            gbuf[b][...] = (pr * (tbuf[b][...] - delta)).astype(BF)

        def grads(i, b):
            scale = HEAD_DIM ** -0.5
            dqkv[w, :, lanes(i)] = (unstack(dot_nn(gbuf[b][...], qkv[:, lanes(i, D)])) * scale).astype(BF)
            dkvt[lanes(i), :] += dot_tn(stack(qkv[rows, lanes(i)]) * scale, gbuf[b][...])
            dkvt[lanes(i, D), :] += dot_tn(stack(da[:, lanes(i)]), pbuf[b][...])

        pair_pipeline(scores, slopes, grads)

        @pl.loop(0, 2 * pairs)
        def _(i):
            dqkv[w, :, lanes(i, D)] = dkvt[lanes(i), rows].T.astype(BF)

        put(5, p, dqkv.at[w], dqkv_o).start()
        for c in range(3):
            arrived((c + 9) % RING)
        dn = dot_nn(dqkv[w, :, 0:CH], ring[9 % RING])
        for c in range(1, 3):
            dn = dn + dot_nn(dqkv[w, :, c * CH:(c + 1) * CH], ring[(c + 9) % RING])
        acc[...] = dn
        for c in range(3):
            fetch_next(c + 9)
        dh, dg = norm_grad(acc[...], hin[p], gain0)
        dgain_ref[0:1, :] += dg

        @pl.when(me > 0)
        def _():
            @pl.when(me < last)
            def _():
                fwd_copy(p).wait_send()
            hs[p] = (dhm[w].astype(F32) + dh).astype(BF)
            bwd_copy(p).start()
        return carry

    def backward(tb0, tb1, gb0, gb1, db0, db1, du, dqkv, dhm, da, dkvt):
        dkvt[...] = jnp.zeros_like(dkvt)
        bufs = ((tb0, tb1), (gb0, gb1), (db0, db1), du, dqkv, dhm, da, dkvt)
        lax.fori_loop(0, pieces, functools.partial(bwd_piece, bufs), 0)
        for e in range(2):
            put(4, e, du.at[1 - e], du_o).wait()
            put(5, e, dqkv.at[1 - e], dqkv_o).wait()
            put(6, e, dhm.at[1 - e], dhm_o).wait()

    wide, tight, part = pltpu.VMEM((2 * ROWS, seq), F32), pltpu.VMEM((2 * ROWS, seq), BF), pltpu.VMEM((ROWS, D), F32)
    pl.run_scoped(backward, wide, wide, tight, tight, part, part,
                  pltpu.VMEM((2, ROWS, 4 * CH), BF), pltpu.VMEM((2, ROWS, 3 * CH), BF), pltpu.VMEM((2, ROWS, D), BF),
                  pltpu.VMEM((ROWS, D), BF), pltpu.VMEM((2 * D, seq), F32))
    loss_ref[...] = loss_in[...]

    for p in range(pieces):
        put(1, p, att.at[p], a_o).wait()
        put(7, p, dho.at[p], dho_o).wait()

        @pl.when(me == 0)
        def _():
            fwd_copy(p).wait_send()

        @pl.when(me > 0)
        def _():
            bwd_copy(p).wait_send()
    for e in range(2):
        p = pieces - 2 + e
        put(0, p, n1.at[e], n1_o).wait()
        put(2, p, n2.at[e], n2_o).wait()
        put(3, p, act.at[e], act_o).wait()

    @pl.when(me > 0)
    def _():
        loss_copy().wait_send()


def run_pipeline(stages, x, y, w_qkv, w_out, w_up, w_down, gain):
    seq, width = x.shape[1], x.shape[2]
    ffn = w_up.shape[2]
    pieces = seq // ROWS
    hbm = pl.BlockSpec(memory_space=pl.ANY)
    vmem = pl.BlockSpec(memory_space=pltpu.VMEM)
    V = pltpu.VMEM
    full = V((pieces, ROWS, width), BF)
    two = V((2, ROWS, width), BF)
    wide = V((2 * ROWS, seq), F32)
    tight = V((2 * ROWS, seq), BF)
    widths = (width, width, width, ffn, ffn, 3 * width, width, width)
    outs = [jax.ShapeDtypeStruct((8, 128), F32), jax.ShapeDtypeStruct((2, width), F32)]
    outs += [jax.ShapeDtypeStruct((seq, w), BF) for w in widths]
    outs += [jax.ShapeDtypeStruct((CHUNKS, width, width), BF)]
    dma = pltpu.SemaphoreType.DMA
    return pl.pallas_call(
        functools.partial(pipeline_kernel, stages, seq, width),
        out_shape=outs,
        in_specs=[hbm] * 6 + [vmem],
        out_specs=[vmem, vmem] + [hbm] * 9,
        scratch_shapes=[
            V((RING, width, width), BF),
            full, full, full,
            two, full, two,
            V((seq, 3 * width), BF),
            V((seq, ffn), F32),
            V((2, ROWS, ffn), BF),
            V((ROWS, width), F32),
            full,
            wide, V((8, 128), F32),
            wide, wide, tight, tight,
            dma((RING,)), dma((5,)), dma((3,)), dma((pieces,)), dma((8, pieces)),
            dma((pieces,)), dma((pieces,)), dma((pieces,)), dma((pieces,)), dma((1,)), dma((1,)),
        ],
        compiler_params=pltpu.CompilerParams(collective_id=0, has_side_effects=True, vmem_limit_bytes=67043328),
        name='pipeline',
    )(x, y, w_qkv, w_out, w_up, w_down, gain)


def wgrad_kernel(n1, dqkv, att, dhm, n2, du, act, dho, g_qkv, g_out, g_up, g_down,
                 n1v, dqkvv, attv, dhmv, n2v, duv, actv, dhov, stage, isem, osem):
    D = n1.shape[1]
    T = stage.shape[2]
    loads = ((att, attv), (dhm, dhmv), (dho, dhov), (act, actv), (n2, n2v), (du, duv), (n1, n1v), (dqkv, dqkvv))
    copies = [pltpu.make_async_copy(src, dst, isem.at[i]) for i, (src, dst) in enumerate(loads)]
    for c in copies:
        c.start()

    def tile(g, r, c):
        return g.at[0, pl.ds(pl.multiple_of(r * D, D), D), pl.ds(pl.multiple_of(c * T, T), T)]

    def section(base, left, right, g, rows, cols):
        def step(i, carry):
            slot = lax.rem(base + i, STAGES)
            r, c = lax.div(i, cols), lax.rem(i, cols)

            @pl.when(base + i >= STAGES)
            def _():
                pltpu.make_async_copy(stage.at[slot], tile(g_out, 0, 0), osem.at[slot]).wait()
            a = left[:, pl.ds(pl.multiple_of(r * D, D), D)]
            stage[slot] = dot_tn(a, right[:, pl.ds(pl.multiple_of(c * T, T), T)])
            pltpu.make_async_copy(stage.at[slot], tile(g, r, c), osem.at[slot]).start()
            return carry
        lax.fori_loop(0, rows * cols, step, 0)
        return base + rows * cols

    base = 0
    for pair, left, right, g in ((0, attv, dhmv, g_out), (2, actv, dhov, g_down), (4, n2v, duv, g_up), (6, n1v, dqkvv, g_qkv)):
        if pair != 2:
            copies[pair].wait()
            copies[pair + 1].wait()
        else:
            copies[2].wait()
            copies[3].wait()
        base = section(base, left, right, g, left.shape[1] // D, right.shape[1] // T)
    for slot in range(STAGES):
        pltpu.make_async_copy(stage.at[slot], tile(g_out, 0, 0), osem.at[slot]).wait()


def weight_grads(n1, dqkv, att, dhm, n2, du, act, dho):
    D = n1.shape[1]
    hbm = pl.BlockSpec(memory_space=pl.ANY)
    ins = (n1, dqkv, att, dhm, n2, du, act, dho)
    shapes = ((D, dqkv.shape[1]), (D, D), (D, du.shape[1]), (act.shape[1], D))
    dma = pltpu.SemaphoreType.DMA
    return pl.pallas_call(
        wgrad_kernel,
        out_shape=[jax.ShapeDtypeStruct((1,) + sh, F32) for sh in shapes],
        in_specs=[hbm] * 8,
        out_specs=[hbm] * 4,
        scratch_shapes=[pltpu.VMEM(a.shape, BF) for a in ins] + [pltpu.VMEM((STAGES, D, D // 2), F32), dma((8,)), dma((STAGES,))],
        compiler_params=pltpu.CompilerParams(vmem_limit_bytes=60 * 2 ** 20),
        name='weight_grads',
    )(*ins)


def solution(mesh):
    stages = mesh.shape['stage']

    def per_device(x, y, w_qkv, w_out, w_up, w_down, norm_gain):
        loss, dgain, n1, att, n2, act, du, dqkv, dhm, dho, _ = run_pipeline(stages, x, y, w_qkv, w_out, w_up, w_down, norm_gain)
        g_qkv, g_out, g_up, g_down = weight_grads(n1, dqkv, att, dhm, n2, du, act, dho)
        return loss[0, 0].reshape(1), g_qkv, g_out, g_up, g_down, dgain[None]

    weight_spec = P('stage')
    grad_spec = P(('data', 'stage'))
    return jax.shard_map(per_device, mesh=mesh, in_specs=(P('data'), P('data')) + (weight_spec,) * 5,
                         out_specs=(P('data'),) + (grad_spec,) * 5, check_vma=False)
```

```python
import functools
import math

import jax
import jax.numpy as jnp
from jax import lax
from jax.experimental import pallas as pl
from jax.experimental.pallas import tpu as pltpu
from jax.sharding import PartitionSpec as P

MESH = pl.DeviceIdType.MESH
BF = jnp.bfloat16
F32 = jnp.float32
HEAD_DIM = 64
ROWS = 128
RING = 6
CHUNKS = 12
STAGES = 3
EPS = 1e-6
GELU_C = math.sqrt(2.0 / math.pi)
GELU_A = 0.044715
LOG2E = math.log2(math.e)


def dot_nn(a, b):
    return jnp.dot(a, b, preferred_element_type=F32)


def dot_nt(a, b):
    return lax.dot_general(a, b, (((1,), (1,)), ((), ())), preferred_element_type=F32)


def dot_tn(a, b):
    return lax.dot_general(a, b, (((0,), (0,)), ((), ())), preferred_element_type=F32)


def norm_stats(h_bf):
    h = h_bf.astype(F32)
    inv = lax.rsqrt(jnp.mean(h * h, axis=-1, keepdims=True) + EPS)
    return h, inv


def norm_grad(dn, h_bf, gain):
    h, inv = norm_stats(h_bf)
    hhat = h * inv
    dgain = jnp.sum(dn * hhat, axis=0, keepdims=True)
    dhhat = dn * gain
    corr = jnp.mean(dhhat * hhat, axis=-1, keepdims=True)
    return inv * (dhhat - hhat * corr), dgain


def gelu_parts(u):
    u2 = u * u
    t = jnp.tanh(u * (GELU_C + (GELU_C * GELU_A) * u2))
    return u2, t


def pipeline_kernel(stages, seq, width, x_ref, y_ref, wqkv, wout, wup, wdown, gain_ref,
                    loss_ref, dgain_ref, n1_o, a_o, n2_o, act_o, du_o, dqkv_o, dhm_o, dho_o, wt,
                    ring, hin, hs, hmid, n1, att, n2, qkv, u_buf, act, acc, dho, bias, loss_in,
                    sb0, sb1, pb0, pb1, lse,
                    wsem, esem, tsem, xsem, osem, fs, fr, bs, br, ls, lr):
    me = lax.axis_index('stage')
    data = lax.axis_index('data')
    last = stages - 1
    half = stages // 2
    right = lax.rem(me + 1, stages)
    left = lax.rem(me + stages - 1, stages)
    D = width
    CH = D
    LN = 2 * HEAD_DIM
    pairs = D // LN
    pieces = seq // ROWS
    count = float(seq * width)
    sbuf, pbuf = (sb0, sb1), (pb0, pb1)

    def fetch(kind, j, slot, extra=None):
        cols = pl.ds(pl.multiple_of(j * CH, CH), CH)
        src = {'q': lambda: wqkv.at[0, :, cols], 'o': lambda: wout.at[0], 'u': lambda: wup.at[0, :, cols], 'd': lambda: wdown.at[0, cols, :]}[kind]()
        if extra is None:
            pltpu.make_async_copy(src, ring.at[slot], wsem.at[slot]).start()
        else:
            pltpu.make_async_copy(src, extra.at[slot], esem.at[slot]).start()

    def fetch_bwd(idx):
        slot = lax.rem(idx, RING)
        pltpu.make_async_copy(wt.at[idx], ring.at[slot], wsem.at[slot]).start()

    def arrived(slot):
        pltpu.make_async_copy(wout.at[0], ring.at[slot], wsem.at[slot]).wait()

    def put(idx, p, buf, out):
        return pltpu.make_async_copy(buf, out.at[pl.ds(pl.multiple_of(p * ROWS, ROWS), ROWS)], osem.at[idx, p])

    def fwd_copy(p):
        return pltpu.make_async_remote_copy(src_ref=hs.at[p], dst_ref=hin.at[p], send_sem=fs.at[p], recv_sem=fr.at[p],
                                            device_id=(data, right), device_id_type=MESH)

    def bwd_copy(p):
        return pltpu.make_async_remote_copy(src_ref=hs.at[p], dst_ref=dho.at[p], send_sem=bs.at[p], recv_sem=br.at[p],
                                            device_id=(data, left), device_id_type=MESH)

    def loss_copy():
        return pltpu.make_async_remote_copy(src_ref=loss_in, dst_ref=loss_in, send_sem=ls.at[0], recv_sem=lr.at[0],
                                            device_id=(data, left), device_id_type=MESH)

    def transpose_weights():
        def fetch_any(b):
            slot = lax.rem(b, 3)
            for odd, kind in ((0, 'd'), (1, 'u')):
                @pl.when((b < 8) & (lax.rem(b, 2) == odd))
                def _(kind=kind):
                    fetch(kind, lax.div(b, 2), slot)

            @pl.when(b == 8)
            def _():
                fetch('o', 0, slot)

            @pl.when(b > 8)
            def _():
                fetch('q', b - 9, slot)

        def store(b):
            slot = lax.rem(b, 3)
            return pltpu.make_async_copy(ring.at[slot + 3], wt.at[b], tsem.at[slot])

        fetch_any(0)
        fetch_any(1)

        @pl.loop(0, CHUNKS)
        def _(b):
            slot = lax.rem(b, 3)

            @pl.when(b + 2 < CHUNKS)
            def _():
                fetch_any(b + 2)
            arrived(slot)

            @pl.when(b >= 3)
            def _():
                store(b - 3).wait()

            @pl.loop(0, D // 256)
            def _(r):
                blk = pl.ds(pl.multiple_of(r * 256, 256), 256)
                ring[slot + 3, :, blk] = ring[slot, blk, :].T
            store(b).start()

        @pl.loop(CHUNKS - 3, CHUNKS)
        def _(b):
            store(b).wait()

    def start_fwd(extra):
        for c in range(3):
            fetch('q', c, c)
        fetch('o', 0, 3)
        fetch('u', 0, 4)
        fetch('d', 0, 5)
        for e, (kind, j) in enumerate((('u', 1), ('d', 1), ('u', 2), ('d', 2), ('d', 3))):
            fetch(kind, j, e, extra)

    @pl.when(me == 0)
    def _():
        for p in range(pieces):
            pltpu.make_async_copy(x_ref.at[0, pl.ds(p * ROWS, ROWS)], hin.at[p], xsem.at[p]).start()

    @pl.when(me == last)
    def _():
        for p in range(pieces):
            pltpu.make_async_copy(y_ref.at[0, pl.ds(p * ROWS, ROWS)], dho.at[p], xsem.at[p]).start()

    barrier = pltpu.get_barrier_semaphore()
    for nb in (left, right):
        pl.semaphore_signal(barrier, inc=1, device_id=(data, nb), device_id_type=MESH)
    pl.semaphore_wait(barrier, 2)

    @pl.when(me >= half)
    def _():
        transpose_weights()

    dgain_ref[...] = jnp.zeros_like(dgain_ref)

    @pl.when(me == last)
    def _():
        loss_in[...] = jnp.zeros_like(loss_in)
    gain0 = gain_ref[0, 0:1, :].astype(F32)
    gain1 = gain_ref[0, 1:2, :].astype(F32)
    low = lax.broadcasted_iota(jnp.int32, (ROWS, LN), 1) < HEAD_DIM

    def stack(a):
        zero = jnp.zeros_like(a)
        return jnp.concatenate([jnp.where(low, a, zero), jnp.where(low, zero, a)], axis=0)

    def unstack(a):
        return jnp.where(low, a[:ROWS], a[ROWS:])

    def lanes(i, base=0):
        return pl.ds(pl.multiple_of(i * LN, LN) + base, LN)

    r = lax.rem(lax.broadcasted_iota(jnp.int32, (2 * ROWS, ROWS), 0), ROWS)
    c = lax.broadcasted_iota(jnp.int32, (2 * ROWS, ROWS), 1)
    bias[...] = jnp.where(c <= r, 0.0, -1e30)

    lane = lax.broadcasted_iota(jnp.int32, (2 * ROWS, 128), 1)

    def masked(s):
        s = s * (HEAD_DIM ** -0.5 * LOG2E)
        keys = s.shape[1]
        if keys > ROWS:
            return jnp.concatenate([s[:, :keys - ROWS], s[:, keys - ROWS:] + bias[...]], axis=1)
        return s + bias[...]

    def by_piece(p, body):
        for k in range(pieces):
            @pl.when(p == k)
            def _(k=k):
                body((k + 1) * ROWS)

    def pair_pipeline(first, middle, final):
        first(0, 0)

        @pl.loop(0, pairs // 2)
        def _(h):
            i = 2 * h
            first(i + 1, 1)
            middle(i, 0)
            final(jnp.maximum(i - 1, 0), 1)
            first(jnp.minimum(i + 2, pairs - 1), 0)
            middle(i + 1, 1)
            final(i, 0)
        final(pairs - 1, 1)

    def fwd_piece(extra, p, carry):
        row0 = pl.multiple_of(p * ROWS, ROWS)
        rows = pl.ds(row0, ROWS)
        w = lax.rem(p, 2)

        @pl.when(p >= 2)
        def _():
            put(0, p - 2, n1.at[w], n1_o).wait()
            put(2, p - 2, n2.at[w], n2_o).wait()
            put(3, p - 2, act.at[w], act_o).wait()

        @pl.when(me == 0)
        def _():
            pltpu.make_async_copy(x_ref.at[0, rows], hin.at[p], xsem.at[p]).wait()

        @pl.when(me > 0)
        def _():
            fwd_copy(p).wait_recv()

        @pl.when(p == 0)
        def _():
            for c in range(3):
                arrived(c)

        turn = (p == pieces - 1) & (me >= half)

        h, inv = norm_stats(hin[p])
        n1[w] = (h * inv * gain0).astype(BF)
        put(0, p, n1.at[w], n1_o).start()

        for c in range(3):
            qkv[rows, c * CH:(c + 1) * CH] = dot_nn(n1[w], ring[c]).astype(BF)

        @pl.when(turn)
        def _():
            for c in range(3):
                fetch_bwd(c)

        def attend(keys):
            def scores(i, b):
                sbuf[b][:, :keys] = dot_nt(stack(qkv[rows, lanes(i)]), qkv[:keys, lanes(i, D)])

            def softmax(i, b):
                s = masked(sbuf[b][:, :keys])
                top = jnp.max(s, axis=-1, keepdims=True)
                e = jnp.exp2(s - top)
                total = jnp.sum(e, axis=-1, keepdims=True)
                lse[p] = jnp.where(lane == i, top + jnp.log2(total), lse[p])
                pbuf[b][:, :keys] = (e * (1.0 / total)).astype(BF)

            def mix(i, b):
                att[p, :, lanes(i)] = unstack(dot_nn(pbuf[b][:, :keys], qkv[:keys, lanes(i, 2 * D)])).astype(BF)

            pair_pipeline(scores, softmax, mix)

        by_piece(p, attend)
        put(1, p, att.at[p], a_o).start()
        arrived(3)
        hmid[p] = (hin[p].astype(F32) + dot_nn(att[p], ring[3])).astype(BF)
        fetch('u', 3, 3)
        h, inv = norm_stats(hmid[p])
        n2[w] = (h * inv * gain1).astype(BF)
        put(2, p, n2.at[w], n2_o).start()

        @pl.when(p == 0)
        def _():
            arrived(4)
            arrived(5)
            for e in range(5):
                pltpu.make_async_copy(wout.at[0], extra.at[e], esem.at[e]).wait()

        def up(j, weight):
            u_buf[rows, j * CH:(j + 1) * CH] = dot_nn(n2[w], weight[...])

        def down(j, weight):
            u = u_buf[rows, j * CH:(j + 1) * CH]
            u2, t = gelu_parts(u)
            act[w, :, j * CH:(j + 1) * CH] = (0.5 * u * (1.0 + t)).astype(BF)
            return dot_nn(act[w, :, j * CH:(j + 1) * CH], weight[...])

        up(0, ring.at[4])
        up(1, extra.at[0])
        acc[...] = hmid[p].astype(F32) + down(0, ring.at[5])
        up(2, extra.at[2])
        acc[...] += down(1, extra.at[1])
        arrived(3)
        up(3, ring.at[3])
        acc[...] += down(2, extra.at[3])
        hs[p] = (acc[...] + down(3, extra.at[4])).astype(BF)

        @pl.when(me < last)
        def _():
            fwd_copy(p).start()

        put(3, p, act.at[w], act_o).start()

        @pl.when(p < pieces - 1)
        def _():
            fetch('o', 0, 3)

        @pl.when(turn)
        def _():
            for b in range(3, RING):
                fetch_bwd(b)

        @pl.when(me == last)
        def _():
            pltpu.make_async_copy(y_ref.at[0, rows], dho.at[p], xsem.at[p]).wait()
            err = hs[p].astype(F32) - dho[p].astype(F32)
            dho[p] = (err / count).astype(BF)
            part = jnp.sum(jnp.sum(err * err, axis=0, keepdims=True), axis=1, keepdims=True)
            loss_in[...] += part * (0.5 / count)
        return carry

    def forward(extra):
        start_fwd(extra)
        lax.fori_loop(0, pieces, functools.partial(fwd_piece, extra), 0)

    pl.run_scoped(forward, pltpu.VMEM((5, D, D), BF))

    @pl.when(me < half)
    def _():
        transpose_weights()
        for b in range(RING):
            fetch_bwd(b)
    def bwd_piece(bufs, t, carry):
        gbuf, dbuf, du, dqkv, dhm, da, dkvt = bufs
        p = pieces - 1 - t
        row0 = pl.multiple_of(p * ROWS, ROWS)
        rows = pl.ds(row0, ROWS)
        w = lax.rem(t, 2)

        @pl.when(t >= 2)
        def _():
            put(4, p + 2, du.at[w], du_o).wait()
            put(5, p + 2, dqkv.at[w], dqkv_o).wait()
            put(6, p + 2, dhm.at[w], dhm_o).wait()

        @pl.when(me < last)
        def _():
            bwd_copy(p).wait_recv()

        @pl.when((me < last) & (t == 0))
        def _():
            loss_copy().wait_recv()

        @pl.when((me > 0) & (t == 0))
        def _():
            loss_copy().start()
        put(7, p, dho.at[p], dho_o).start()

        def fetch_next(idx):
            nxt = idx + RING
            if nxt < CHUNKS:
                fetch_bwd(nxt)
            else:
                @pl.when(t < pieces - 1)
                def _():
                    fetch_bwd(nxt - CHUNKS)

        def back_down(j):
            arrived(2 * j % RING)
            dbuf[j % 2][...] = dot_nn(dho[p], ring[2 * j % RING])

        def back_up(j):
            cols = slice(j * CH, (j + 1) * CH)
            u = u_buf[rows, cols]
            u2, th = gelu_parts(u)
            slope = 0.5 * (1.0 + th) + (0.5 * u) * (1.0 - th * th) * (GELU_C + (3.0 * GELU_C * GELU_A) * u2)
            du[w, :, cols] = (dbuf[j % 2][...] * slope).astype(BF)
            return dot_nn(du[w, :, cols], ring[(2 * j + 1) % RING])

        back_down(0)
        fetch_next(0)
        for j in range(4):
            arrived((2 * j + 1) % RING)
            if j < 3:
                back_down(j + 1)
            part = back_up(j)
            if j == 0:
                acc[...] = part
            else:
                acc[...] += part
            fetch_next(2 * j + 1)
            if j < 3:
                fetch_next(2 * j + 2)

        put(4, p, du.at[w], du_o).start()
        dh, dg = norm_grad(acc[...], hmid[p], gain1)
        dgain_ref[1:2, :] += dg
        dhm[w] = (dho[p].astype(F32) + dh).astype(BF)
        put(6, p, dhm.at[w], dhm_o).start()
        arrived(8 % RING)
        da[...] = dot_nn(dhm[w], ring[8 % RING]).astype(BF)
        fetch_next(8)

        def attend(keys):
            scale = HEAD_DIM ** -0.5

            def slopes(i, b):
                prod = da[:, lanes(i)].astype(F32) * att[p, :, lanes(i)].astype(F32)
                both = jnp.concatenate([jnp.where(low, prod, 0.0), jnp.where(low, 0.0, prod)], axis=0)
                delta = jnp.sum(both, axis=-1, keepdims=True)
                norm = jnp.sum(jnp.where(lane == i, lse[p], 0.0), axis=-1, keepdims=True)
                pr = jnp.exp2(masked(dot_nt(stack(qkv[rows, lanes(i)]), qkv[:keys, lanes(i, D)])) - norm)
                pbuf[b][:, :keys] = pr.astype(BF)
                dp = dot_nt(stack(da[:, lanes(i)]), qkv[:keys, lanes(i, 2 * D)])
                gbuf[b][:, :keys] = (pr * (dp - delta)).astype(BF)

            def grads(i, b):
                g = gbuf[b][:, :keys]
                dqkv[w, :, lanes(i)] = (unstack(dot_nn(g, qkv[:keys, lanes(i, D)])) * scale).astype(BF)
                dkvt[lanes(i), :keys] += dot_tn(stack(qkv[rows, lanes(i)]) * scale, g)
                dkvt[lanes(i, D), :keys] += dot_tn(stack(da[:, lanes(i)]), pbuf[b][:, :keys])

            slopes(0, 0)

            @pl.loop(0, pairs // 2)
            def _(h):
                slopes(2 * h + 1, 1)
                grads(2 * h, 0)
                slopes(jnp.minimum(2 * h + 2, pairs - 1), 0)
                grads(2 * h + 1, 1)

        by_piece(p, attend)

        @pl.loop(0, 2 * pairs)
        def _(i):
            dqkv[w, :, lanes(i, D)] = dkvt[lanes(i), rows].T.astype(BF)

        put(5, p, dqkv.at[w], dqkv_o).start()
        for c in range(3):
            arrived((c + 9) % RING)
        dn = dot_nn(dqkv[w, :, 0:CH], ring[9 % RING])
        for c in range(1, 3):
            dn = dn + dot_nn(dqkv[w, :, c * CH:(c + 1) * CH], ring[(c + 9) % RING])
        acc[...] = dn
        for c in range(3):
            fetch_next(c + 9)
        dh, dg = norm_grad(acc[...], hin[p], gain0)
        dgain_ref[0:1, :] += dg

        @pl.when(me > 0)
        def _():
            @pl.when(me < last)
            def _():
                fwd_copy(p).wait_send()
            hs[p] = (dhm[w].astype(F32) + dh).astype(BF)
            bwd_copy(p).start()
        return carry

    def backward(gb0, gb1, db0, db1, du, dqkv, dhm, da, dkvt):
        dkvt[...] = jnp.zeros_like(dkvt)
        bufs = ((gb0, gb1), (db0, db1), du, dqkv, dhm, da, dkvt)
        lax.fori_loop(0, pieces, functools.partial(bwd_piece, bufs), 0)
        for e in range(2):
            put(4, e, du.at[1 - e], du_o).wait()
            put(5, e, dqkv.at[1 - e], dqkv_o).wait()
            put(6, e, dhm.at[1 - e], dhm_o).wait()

    tight, part = pltpu.VMEM((2 * ROWS, seq), BF), pltpu.VMEM((ROWS, D), F32)
    pl.run_scoped(backward, tight, tight, part, part,
                  pltpu.VMEM((2, ROWS, 4 * CH), BF), pltpu.VMEM((2, ROWS, 3 * CH), BF), pltpu.VMEM((2, ROWS, D), BF),
                  pltpu.VMEM((ROWS, D), BF), pltpu.VMEM((2 * D, seq), F32))
    loss_ref[...] = loss_in[...]

    for p in range(pieces):
        put(1, p, att.at[p], a_o).wait()
        put(7, p, dho.at[p], dho_o).wait()

        @pl.when(me == 0)
        def _():
            fwd_copy(p).wait_send()

        @pl.when(me > 0)
        def _():
            bwd_copy(p).wait_send()
    for e in range(2):
        p = pieces - 2 + e
        put(0, p, n1.at[e], n1_o).wait()
        put(2, p, n2.at[e], n2_o).wait()
        put(3, p, act.at[e], act_o).wait()

    @pl.when(me > 0)
    def _():
        loss_copy().wait_send()


def run_pipeline(stages, x, y, w_qkv, w_out, w_up, w_down, gain):
    seq, width = x.shape[1], x.shape[2]
    ffn = w_up.shape[2]
    pieces = seq // ROWS
    hbm = pl.BlockSpec(memory_space=pl.ANY)
    vmem = pl.BlockSpec(memory_space=pltpu.VMEM)
    V = pltpu.VMEM
    full = V((pieces, ROWS, width), BF)
    two = V((2, ROWS, width), BF)
    wide = V((2 * ROWS, seq), F32)
    tight = V((2 * ROWS, seq), BF)
    widths = (width, width, width, ffn, ffn, 3 * width, width, width)
    outs = [jax.ShapeDtypeStruct((8, 128), F32), jax.ShapeDtypeStruct((2, width), F32)]
    outs += [jax.ShapeDtypeStruct((seq, w), BF) for w in widths]
    outs += [jax.ShapeDtypeStruct((CHUNKS, width, width), BF)]
    dma = pltpu.SemaphoreType.DMA
    return pl.pallas_call(
        functools.partial(pipeline_kernel, stages, seq, width),
        out_shape=outs,
        in_specs=[hbm] * 6 + [vmem],
        out_specs=[vmem, vmem] + [hbm] * 9,
        scratch_shapes=[
            V((RING, width, width), BF),
            full, full, full,
            two, full, two,
            V((seq, 3 * width), BF),
            V((seq, ffn), F32),
            V((2, ROWS, ffn), BF),
            V((ROWS, width), F32),
            full,
            V((2 * ROWS, ROWS), F32), V((8, 128), F32),
            wide, wide, tight, tight, V((pieces, 2 * ROWS, 128), F32),
            dma((RING,)), dma((5,)), dma((3,)), dma((pieces,)), dma((8, pieces)),
            dma((pieces,)), dma((pieces,)), dma((pieces,)), dma((pieces,)), dma((1,)), dma((1,)),
        ],
        compiler_params=pltpu.CompilerParams(collective_id=0, has_side_effects=True, vmem_limit_bytes=67043328),
        name='pipeline',
    )(x, y, w_qkv, w_out, w_up, w_down, gain)


def wgrad_kernel(n1, dqkv, att, dhm, n2, du, act, dho, loss, dgain, g_qkv, g_out, g_up, g_down, g_gain, loss_out,
                 n1v, dqkvv, attv, dhmv, n2v, duv, actv, dhov, stage, dgv, lossv, isem, osem, ssem):
    D = n1.shape[1]
    T = stage.shape[2]
    loads = ((att, attv), (dhm, dhmv), (dho, dhov), (act, actv), (n2, n2v), (du, duv), (n1, n1v), (dqkv, dqkvv))
    copies = [pltpu.make_async_copy(src, dst, isem.at[i]) for i, (src, dst) in enumerate(loads)]
    for c in copies:
        c.start()
    small_in = [pltpu.make_async_copy(src, dst, ssem.at[i]) for i, (src, dst) in enumerate(((dgain, dgv), (loss.at[0:1], lossv)))]
    small_out = [pltpu.make_async_copy(src, dst, ssem.at[2 + i]) for i, (src, dst) in enumerate(((dgv, g_gain.at[0]), (lossv, loss_out)))]
    for c in small_in:
        c.start()

    def tile(g, r, c):
        return g.at[0, pl.ds(pl.multiple_of(r * D, D), D), pl.ds(pl.multiple_of(c * T, T), T)]

    def section(base, left, right, g, rows, cols):
        def step(i, carry):
            slot = lax.rem(base + i, STAGES)
            r, c = lax.div(i, cols), lax.rem(i, cols)

            @pl.when(base + i >= STAGES)
            def _():
                pltpu.make_async_copy(stage.at[slot], tile(g_out, 0, 0), osem.at[slot]).wait()
            a = left[:, pl.ds(pl.multiple_of(r * D, D), D)]
            stage[slot] = dot_tn(a, right[:, pl.ds(pl.multiple_of(c * T, T), T)])
            pltpu.make_async_copy(stage.at[slot], tile(g, r, c), osem.at[slot]).start()
            return carry
        lax.fori_loop(0, rows * cols, step, 0)
        return base + rows * cols

    base = 0
    for pair, left, right, g in ((0, attv, dhmv, g_out), (2, actv, dhov, g_down), (4, n2v, duv, g_up), (6, n1v, dqkvv, g_qkv)):
        if pair != 2:
            copies[pair].wait()
            copies[pair + 1].wait()
        else:
            copies[2].wait()
            copies[3].wait()
        base = section(base, left, right, g, left.shape[1] // D, right.shape[1] // T)
    for a, b in zip(small_in, small_out):
        a.wait()
        b.start()
    for b in small_out:
        b.wait()
    for slot in range(STAGES):
        pltpu.make_async_copy(stage.at[slot], tile(g_out, 0, 0), osem.at[slot]).wait()


def weight_grads(n1, dqkv, att, dhm, n2, du, act, dho, loss, dgain):
    D = n1.shape[1]
    hbm = pl.BlockSpec(memory_space=pl.ANY)
    ins = (n1, dqkv, att, dhm, n2, du, act, dho)
    shapes = ((D, dqkv.shape[1]), (D, D), (D, du.shape[1]), (act.shape[1], D))
    dma = pltpu.SemaphoreType.DMA
    return pl.pallas_call(
        wgrad_kernel,
        out_shape=[jax.ShapeDtypeStruct((1,) + sh, F32) for sh in shapes + (dgain.shape,)] + [jax.ShapeDtypeStruct((1, 128), F32)],
        in_specs=[hbm] * 10,
        out_specs=[hbm] * 6,
        scratch_shapes=[pltpu.VMEM(a.shape, BF) for a in ins] + [pltpu.VMEM((STAGES, D, D // 2), F32), pltpu.VMEM(dgain.shape, F32), pltpu.VMEM((1, 128), F32),
                                                                dma((8,)), dma((STAGES,)), dma((4,))],
        compiler_params=pltpu.CompilerParams(vmem_limit_bytes=60 * 2 ** 20),
        name='weight_grads',
    )(*ins, loss, dgain)


def solution(mesh):
    stages = mesh.shape['stage']

    def per_device(x, y, w_qkv, w_out, w_up, w_down, norm_gain):
        loss, dgain, n1, att, n2, act, du, dqkv, dhm, dho, _ = run_pipeline(stages, x, y, w_qkv, w_out, w_up, w_down, norm_gain)
        g_qkv, g_out, g_up, g_down, g_gain, loss = weight_grads(n1, dqkv, att, dhm, n2, du, act, dho, loss, dgain)
        return loss[0, :1], g_qkv, g_out, g_up, g_down, g_gain

    weight_spec = P('stage')
    grad_spec = P(('data', 'stage'))
    return jax.shard_map(per_device, mesh=mesh, in_specs=(P('data'), P('data')) + (weight_spec,) * 5,
                         out_specs=(P('data'),) + (grad_spec,) * 5, check_vma=False)
```

```python
import functools
import math

import jax
import jax.numpy as jnp
from jax import lax
from jax.experimental import pallas as pl
from jax.experimental.pallas import tpu as pltpu
from jax.sharding import PartitionSpec as P

MESH = pl.DeviceIdType.MESH
BF = jnp.bfloat16
F32 = jnp.float32
HEAD_DIM = 64
ROWS = 128
RING = 6
CHUNKS = 12
STAGES = 5
EPS = 1e-6
GELU_C = math.sqrt(2.0 / math.pi)
GELU_A = 0.044715
LOG2E = math.log2(math.e)


def dot_nn(a, b):
    return jnp.dot(a, b, preferred_element_type=F32)


def dot_nt(a, b):
    return lax.dot_general(a, b, (((1,), (1,)), ((), ())), preferred_element_type=F32)


def dot_tn(a, b):
    return lax.dot_general(a, b, (((0,), (0,)), ((), ())), preferred_element_type=F32)


def norm_stats(h_bf):
    h = h_bf.astype(F32)
    inv = lax.rsqrt(jnp.mean(h * h, axis=-1, keepdims=True) + EPS)
    return h, inv


def norm_grad(dn, h_bf, gain):
    h, inv = norm_stats(h_bf)
    hhat = h * inv
    dgain = jnp.sum(dn * hhat, axis=0, keepdims=True)
    dhhat = dn * gain
    corr = jnp.mean(dhhat * hhat, axis=-1, keepdims=True)
    return inv * (dhhat - hhat * corr), dgain


def gelu_parts(u):
    u2 = u * u
    t = jnp.tanh(u * (GELU_C + (GELU_C * GELU_A) * u2))
    return u2, t


def pipeline_kernel(stages, seq, width, x_ref, y_ref, wqkv, wout, wup, wdown, gain_ref,
                    loss_ref, dgain_ref, n1_o, a_o, n2_o, act_o, du_o, dqkv_o, dhm_o, dho_o, wt,
                    ring, hin, hs, hmid, n1, att, n2, qkv, u_buf, act, acc, dho, bias, loss_in,
                    sb0, sb1, pb0, pb1, lse,
                    wsem, esem, tsem, xsem, osem, fs, fr, bs, br, ls, lr):
    me = lax.axis_index('stage')
    data = lax.axis_index('data')
    last = stages - 1
    half = stages // 2
    right = lax.rem(me + 1, stages)
    left = lax.rem(me + stages - 1, stages)
    D = width
    CH = D
    LN = 2 * HEAD_DIM
    pairs = D // LN
    pieces = seq // ROWS
    count = float(seq * width)
    sbuf, pbuf = (sb0, sb1), (pb0, pb1)

    def fetch(kind, j, slot, extra=None):
        cols = pl.ds(pl.multiple_of(j * CH, CH), CH)
        src = {'q': lambda: wqkv.at[0, :, cols], 'o': lambda: wout.at[0], 'u': lambda: wup.at[0, :, cols], 'd': lambda: wdown.at[0, cols, :]}[kind]()
        if extra is None:
            pltpu.make_async_copy(src, ring.at[slot], wsem.at[slot]).start()
        else:
            pltpu.make_async_copy(src, extra.at[slot], esem.at[slot]).start()

    def fetch_bwd(idx):
        slot = lax.rem(idx, RING)
        pltpu.make_async_copy(wt.at[idx], ring.at[slot], wsem.at[slot]).start()

    def arrived(slot):
        pltpu.make_async_copy(wout.at[0], ring.at[slot], wsem.at[slot]).wait()

    def put(idx, p, buf, out):
        return pltpu.make_async_copy(buf, out.at[pl.ds(pl.multiple_of(p * ROWS, ROWS), ROWS)], osem.at[idx, p])

    def fwd_copy(p):
        return pltpu.make_async_remote_copy(src_ref=hs.at[p], dst_ref=hin.at[p], send_sem=fs.at[p], recv_sem=fr.at[p],
                                            device_id=(data, right), device_id_type=MESH)

    def bwd_copy(p):
        return pltpu.make_async_remote_copy(src_ref=hs.at[p], dst_ref=dho.at[p], send_sem=bs.at[p], recv_sem=br.at[p],
                                            device_id=(data, left), device_id_type=MESH)

    def loss_copy():
        return pltpu.make_async_remote_copy(src_ref=loss_in, dst_ref=loss_in, send_sem=ls.at[0], recv_sem=lr.at[0],
                                            device_id=(data, left), device_id_type=MESH)

    def transpose_weights():
        def fetch_any(b):
            slot = lax.rem(b, 3)
            for odd, kind in ((0, 'd'), (1, 'u')):
                @pl.when((b < 8) & (lax.rem(b, 2) == odd))
                def _(kind=kind):
                    fetch(kind, lax.div(b, 2), slot)

            @pl.when(b == 8)
            def _():
                fetch('o', 0, slot)

            @pl.when(b > 8)
            def _():
                fetch('q', b - 9, slot)

        def store(b):
            slot = lax.rem(b, 3)
            return pltpu.make_async_copy(ring.at[slot + 3], wt.at[b], tsem.at[slot])

        fetch_any(0)
        fetch_any(1)

        @pl.loop(0, CHUNKS)
        def _(b):
            slot = lax.rem(b, 3)

            @pl.when(b + 2 < CHUNKS)
            def _():
                fetch_any(b + 2)
            arrived(slot)

            @pl.when(b >= 3)
            def _():
                store(b - 3).wait()

            @pl.loop(0, D // 256)
            def _(r):
                blk = pl.ds(pl.multiple_of(r * 256, 256), 256)
                ring[slot + 3, :, blk] = ring[slot, blk, :].T
            store(b).start()

        @pl.loop(CHUNKS - 3, CHUNKS)
        def _(b):
            store(b).wait()

    def start_fwd(extra):
        for c in range(3):
            fetch('q', c, c)
        fetch('o', 0, 3)
        fetch('u', 0, 4)
        fetch('d', 0, 5)
        for e, (kind, j) in enumerate((('u', 1), ('d', 1), ('u', 2), ('d', 2), ('d', 3))):
            fetch(kind, j, e, extra)

    @pl.when(me == 0)
    def _():
        for p in range(pieces):
            pltpu.make_async_copy(x_ref.at[0, pl.ds(p * ROWS, ROWS)], hin.at[p], xsem.at[p]).start()

    @pl.when(me == last)
    def _():
        for p in range(pieces):
            pltpu.make_async_copy(y_ref.at[0, pl.ds(p * ROWS, ROWS)], dho.at[p], xsem.at[p]).start()

    barrier = pltpu.get_barrier_semaphore()
    for nb in (left, right):
        pl.semaphore_signal(barrier, inc=1, device_id=(data, nb), device_id_type=MESH)
    pl.semaphore_wait(barrier, 2)

    @pl.when(me >= half)
    def _():
        transpose_weights()

    dgain_ref[...] = jnp.zeros_like(dgain_ref)

    @pl.when(me == last)
    def _():
        loss_in[...] = jnp.zeros_like(loss_in)
    gain0 = gain_ref[0, 0:1, :].astype(F32)
    gain1 = gain_ref[0, 1:2, :].astype(F32)
    low = lax.broadcasted_iota(jnp.int32, (ROWS, LN), 1) < HEAD_DIM

    def stack(a):
        zero = jnp.zeros_like(a)
        return jnp.concatenate([jnp.where(low, a, zero), jnp.where(low, zero, a)], axis=0)

    def unstack(a):
        return jnp.where(low, a[:ROWS], a[ROWS:])

    def lanes(i, base=0):
        return pl.ds(pl.multiple_of(i * LN, LN) + base, LN)

    r = lax.rem(lax.broadcasted_iota(jnp.int32, (2 * ROWS, ROWS), 0), ROWS)
    c = lax.broadcasted_iota(jnp.int32, (2 * ROWS, ROWS), 1)
    bias[...] = jnp.where(c <= r, 0.0, -1e30)

    lane = lax.broadcasted_iota(jnp.int32, (2 * ROWS, 128), 1)

    def masked(s):
        s = s * (HEAD_DIM ** -0.5 * LOG2E)
        keys = s.shape[1]
        if keys > ROWS:
            return jnp.concatenate([s[:, :keys - ROWS], s[:, keys - ROWS:] + bias[...]], axis=1)
        return s + bias[...]

    def by_piece(p, body):
        for k in range(pieces):
            @pl.when(p == k)
            def _(k=k):
                body((k + 1) * ROWS)

    def pair_pipeline(first, middle, final):
        first(0, 0)

        @pl.loop(0, pairs // 2)
        def _(h):
            i = 2 * h
            first(i + 1, 1)
            middle(i, 0)
            final(jnp.maximum(i - 1, 0), 1)
            first(jnp.minimum(i + 2, pairs - 1), 0)
            middle(i + 1, 1)
            final(i, 0)
        final(pairs - 1, 1)

    def fwd_piece(extra, p, carry):
        row0 = pl.multiple_of(p * ROWS, ROWS)
        rows = pl.ds(row0, ROWS)
        w = lax.rem(p, 2)

        @pl.when(p >= 2)
        def _():
            put(0, p - 2, n1.at[w], n1_o).wait()
            put(2, p - 2, n2.at[w], n2_o).wait()
            put(3, p - 2, act.at[w], act_o).wait()

        @pl.when(me == 0)
        def _():
            pltpu.make_async_copy(x_ref.at[0, rows], hin.at[p], xsem.at[p]).wait()

        @pl.when(me > 0)
        def _():
            fwd_copy(p).wait_recv()

        @pl.when(p == 0)
        def _():
            for c in range(3):
                arrived(c)

        turn = (p == pieces - 1) & (me >= half)

        h, inv = norm_stats(hin[p])
        n1[w] = (h * inv * gain0).astype(BF)
        put(0, p, n1.at[w], n1_o).start()

        for c in range(3):
            qkv[rows, c * CH:(c + 1) * CH] = dot_nn(n1[w], ring[c]).astype(BF)

        @pl.when(turn)
        def _():
            for c in range(3):
                fetch_bwd(c)

        def attend(keys):
            def scores(i, b):
                sbuf[b][:, :keys] = dot_nt(stack(qkv[rows, lanes(i)]), qkv[:keys, lanes(i, D)])

            def softmax(i, b):
                s = masked(sbuf[b][:, :keys])
                top = jnp.max(s, axis=-1, keepdims=True)
                e = jnp.exp2(s - top)
                total = jnp.sum(e, axis=-1, keepdims=True)
                lse[p] = jnp.where(lane == i, top + jnp.log2(total), lse[p])
                pbuf[b][:, :keys] = (e * (1.0 / total)).astype(BF)

            def mix(i, b):
                att[p, :, lanes(i)] = unstack(dot_nn(pbuf[b][:, :keys], qkv[:keys, lanes(i, 2 * D)])).astype(BF)

            pair_pipeline(scores, softmax, mix)

        by_piece(p, attend)
        put(1, p, att.at[p], a_o).start()
        arrived(3)
        hmid[p] = (hin[p].astype(F32) + dot_nn(att[p], ring[3])).astype(BF)
        fetch('u', 3, 3)
        h, inv = norm_stats(hmid[p])
        n2[w] = (h * inv * gain1).astype(BF)
        put(2, p, n2.at[w], n2_o).start()

        @pl.when(p == 0)
        def _():
            arrived(4)
            arrived(5)
            for e in range(5):
                pltpu.make_async_copy(wout.at[0], extra.at[e], esem.at[e]).wait()

        def up(j, weight):
            u_buf[rows, j * CH:(j + 1) * CH] = dot_nn(n2[w], weight[...])

        def down(j, weight):
            u = u_buf[rows, j * CH:(j + 1) * CH]
            u2, t = gelu_parts(u)
            act[w, :, j * CH:(j + 1) * CH] = (0.5 * u * (1.0 + t)).astype(BF)
            return dot_nn(act[w, :, j * CH:(j + 1) * CH], weight[...])

        up(0, ring.at[4])
        up(1, extra.at[0])
        acc[...] = hmid[p].astype(F32) + down(0, ring.at[5])
        up(2, extra.at[2])
        acc[...] += down(1, extra.at[1])
        arrived(3)
        up(3, ring.at[3])
        acc[...] += down(2, extra.at[3])
        hs[p] = (acc[...] + down(3, extra.at[4])).astype(BF)

        @pl.when(me < last)
        def _():
            fwd_copy(p).start()

        put(3, p, act.at[w], act_o).start()

        @pl.when(p < pieces - 1)
        def _():
            fetch('o', 0, 3)

        @pl.when(turn)
        def _():
            for b in range(3, RING):
                fetch_bwd(b)

        @pl.when(me == last)
        def _():
            pltpu.make_async_copy(y_ref.at[0, rows], dho.at[p], xsem.at[p]).wait()
            err = hs[p].astype(F32) - dho[p].astype(F32)
            dho[p] = (err / count).astype(BF)
            part = jnp.sum(jnp.sum(err * err, axis=0, keepdims=True), axis=1, keepdims=True)
            loss_in[...] += part * (0.5 / count)
        return carry

    def forward(extra):
        start_fwd(extra)
        lax.fori_loop(0, pieces, functools.partial(fwd_piece, extra), 0)

    pl.run_scoped(forward, pltpu.VMEM((5, D, D), BF))

    @pl.when(me < half)
    def _():
        transpose_weights()
        for b in range(RING):
            fetch_bwd(b)
    def bwd_piece(bufs, t, carry):
        gbuf, dbuf, du, dqkv, dhm, da, dkvt = bufs
        p = pieces - 1 - t
        row0 = pl.multiple_of(p * ROWS, ROWS)
        rows = pl.ds(row0, ROWS)
        w = lax.rem(t, 2)

        @pl.when(t >= 2)
        def _():
            put(4, p + 2, du.at[w], du_o).wait()
            put(5, p + 2, dqkv.at[w], dqkv_o).wait()
            put(6, p + 2, dhm.at[w], dhm_o).wait()

        @pl.when(me < last)
        def _():
            bwd_copy(p).wait_recv()

        @pl.when((me < last) & (t == 0))
        def _():
            loss_copy().wait_recv()

        @pl.when((me > 0) & (t == 0))
        def _():
            loss_copy().start()
        put(7, p, dho.at[p], dho_o).start()

        def fetch_next(idx):
            nxt = idx + RING
            if nxt < CHUNKS:
                fetch_bwd(nxt)
            else:
                @pl.when(t < pieces - 1)
                def _():
                    fetch_bwd(nxt - CHUNKS)

        def back_down(j):
            dbuf[j % 2][...] = dot_nn(dho[p], ring[2 * j % RING])

        def back_up(j):
            cols = slice(j * CH, (j + 1) * CH)
            u = u_buf[rows, cols]
            u2, th = gelu_parts(u)
            slope = 0.5 * (1.0 + th) + (0.5 * u) * (1.0 - th * th) * (GELU_C + (3.0 * GELU_C * GELU_A) * u2)
            du[w, :, cols] = (dbuf[j % 2][...] * slope).astype(BF)
            return dot_nn(du[w, :, cols], ring[(2 * j + 1) % RING])

        for idx in range(3):
            arrived(idx)
        back_down(0)
        back_down(1)
        acc[...] = back_up(0)
        for idx in range(3):
            fetch_next(idx)
        for idx in range(3, 6):
            arrived(idx)
        back_down(2)
        acc[...] += back_up(1)
        acc[...] += back_up(2)
        for idx in range(3, 6):
            fetch_next(idx)
        for idx in range(6, 8):
            arrived(idx % RING)
        back_down(3)
        acc[...] += back_up(3)
        for idx in range(6, 8):
            fetch_next(idx)

        put(4, p, du.at[w], du_o).start()
        dh, dg = norm_grad(acc[...], hmid[p], gain1)
        dgain_ref[1:2, :] += dg
        dhm[w] = (dho[p].astype(F32) + dh).astype(BF)
        put(6, p, dhm.at[w], dhm_o).start()
        arrived(8 % RING)
        da[...] = dot_nn(dhm[w], ring[8 % RING]).astype(BF)
        fetch_next(8)

        def attend(keys):
            scale = HEAD_DIM ** -0.5

            def slopes(i, b):
                prod = da[:, lanes(i)].astype(F32) * att[p, :, lanes(i)].astype(F32)
                both = jnp.concatenate([jnp.where(low, prod, 0.0), jnp.where(low, 0.0, prod)], axis=0)
                delta = jnp.sum(both, axis=-1, keepdims=True)
                norm = jnp.sum(jnp.where(lane == i, lse[p], 0.0), axis=-1, keepdims=True)
                pr = jnp.exp2(masked(dot_nt(stack(qkv[rows, lanes(i)]), qkv[:keys, lanes(i, D)])) - norm)
                pbuf[b][:, :keys] = pr.astype(BF)
                dp = dot_nt(stack(da[:, lanes(i)]), qkv[:keys, lanes(i, 2 * D)])
                gbuf[b][:, :keys] = (pr * (dp - delta)).astype(BF)

            def grads(i, b):
                g = gbuf[b][:, :keys]
                dqkv[w, :, lanes(i)] = (unstack(dot_nn(g, qkv[:keys, lanes(i, D)])) * scale).astype(BF)
                dk = dot_tn(stack(qkv[rows, lanes(i)]) * scale, g)
                dv = dot_tn(stack(da[:, lanes(i)]), pbuf[b][:, :keys])
                if keys == seq:
                    dkvt[lanes(i), :] = dk
                    dkvt[lanes(i, D), :] = dv
                else:
                    dkvt[lanes(i), :keys] += dk
                    dkvt[lanes(i, D), :keys] += dv

            slopes(0, 0)

            @pl.loop(0, pairs // 2)
            def _(h):
                slopes(2 * h + 1, 1)
                grads(2 * h, 0)
                slopes(jnp.minimum(2 * h + 2, pairs - 1), 0)
                grads(2 * h + 1, 1)

        by_piece(p, attend)

        @pl.loop(0, 2)
        def _(g):
            for e in range(pairs):
                i = g * pairs + e
                dqkv[w, :, lanes(i, D)] = dkvt[lanes(i), rows].astype(BF).T

        put(5, p, dqkv.at[w], dqkv_o).start()
        for c in range(3):
            arrived((c + 9) % RING)
        dn = dot_nn(dqkv[w, :, 0:CH], ring[9 % RING])
        for c in range(1, 3):
            dn = dn + dot_nn(dqkv[w, :, c * CH:(c + 1) * CH], ring[(c + 9) % RING])
        acc[...] = dn
        for c in range(3):
            fetch_next(c + 9)
        dh, dg = norm_grad(acc[...], hin[p], gain0)
        dgain_ref[0:1, :] += dg

        @pl.when(me > 0)
        def _():
            @pl.when(me < last)
            def _():
                fwd_copy(p).wait_send()
            hs[p] = (dhm[w].astype(F32) + dh).astype(BF)
            bwd_copy(p).start()
        return carry

    def backward(gb0, gb1, db0, db1, du, dqkv, dhm, da, dkvt):
        bufs = ((gb0, gb1), (db0, db1), du, dqkv, dhm, da, dkvt)
        lax.fori_loop(0, pieces, functools.partial(bwd_piece, bufs), 0)
        for e in range(2):
            put(4, e, du.at[1 - e], du_o).wait()
            put(5, e, dqkv.at[1 - e], dqkv_o).wait()
            put(6, e, dhm.at[1 - e], dhm_o).wait()

    tight, part = pltpu.VMEM((2 * ROWS, seq), BF), pltpu.VMEM((ROWS, D), F32)
    pl.run_scoped(backward, tight, tight, part, part,
                  pltpu.VMEM((2, ROWS, 4 * CH), BF), pltpu.VMEM((2, ROWS, 3 * CH), BF), pltpu.VMEM((2, ROWS, D), BF),
                  pltpu.VMEM((ROWS, D), BF), pltpu.VMEM((2 * D, seq), F32))
    loss_ref[...] = loss_in[...]

    for p in range(pieces):
        put(1, p, att.at[p], a_o).wait()
        put(7, p, dho.at[p], dho_o).wait()

        @pl.when(me == 0)
        def _():
            fwd_copy(p).wait_send()

        @pl.when(me > 0)
        def _():
            bwd_copy(p).wait_send()
    for e in range(2):
        p = pieces - 2 + e
        put(0, p, n1.at[e], n1_o).wait()
        put(2, p, n2.at[e], n2_o).wait()
        put(3, p, act.at[e], act_o).wait()

    @pl.when(me > 0)
    def _():
        loss_copy().wait_send()


def run_pipeline(stages, x, y, w_qkv, w_out, w_up, w_down, gain):
    seq, width = x.shape[1], x.shape[2]
    ffn = w_up.shape[2]
    pieces = seq // ROWS
    hbm = pl.BlockSpec(memory_space=pl.ANY)
    vmem = pl.BlockSpec(memory_space=pltpu.VMEM)
    V = pltpu.VMEM
    full = V((pieces, ROWS, width), BF)
    two = V((2, ROWS, width), BF)
    wide = V((2 * ROWS, seq), F32)
    tight = V((2 * ROWS, seq), BF)
    widths = (width, width, width, ffn, ffn, 3 * width, width, width)
    outs = [jax.ShapeDtypeStruct((8, 128), F32), jax.ShapeDtypeStruct((2, width), F32)]
    outs += [jax.ShapeDtypeStruct((seq, w), BF) for w in widths]
    outs += [jax.ShapeDtypeStruct((CHUNKS, width, width), BF)]
    dma = pltpu.SemaphoreType.DMA
    return pl.pallas_call(
        functools.partial(pipeline_kernel, stages, seq, width),
        out_shape=outs,
        in_specs=[hbm] * 6 + [vmem],
        out_specs=[vmem, vmem] + [hbm] * 9,
        scratch_shapes=[
            V((RING, width, width), BF),
            full, full, full,
            two, full, two,
            V((seq, 3 * width), BF),
            V((seq, ffn), F32),
            V((2, ROWS, ffn), BF),
            V((ROWS, width), F32),
            full,
            V((2 * ROWS, ROWS), F32), V((8, 128), F32),
            wide, wide, tight, tight, V((pieces, 2 * ROWS, 128), F32),
            dma((RING,)), dma((5,)), dma((3,)), dma((pieces,)), dma((8, pieces)),
            dma((pieces,)), dma((pieces,)), dma((pieces,)), dma((pieces,)), dma((1,)), dma((1,)),
        ],
        compiler_params=pltpu.CompilerParams(collective_id=0, has_side_effects=True, vmem_limit_bytes=67043328),
        name='pipeline',
    )(x, y, w_qkv, w_out, w_up, w_down, gain)


def wgrad_kernel(n1, dqkv, att, dhm, n2, du, act, dho, loss, dgain, g_qkv, g_out, g_up, g_down, g_gain, loss_out,
                 n1v, dqkvv, attv, dhmv, n2v, duv, actv, dhov, stage, dgv, lossv, isem, osem, ssem):
    D = n1.shape[1]
    T = stage.shape[2]
    loads = ((att, attv), (dhm, dhmv), (dho, dhov), (act, actv), (n2, n2v), (du, duv), (n1, n1v), (dqkv, dqkvv))
    copies = [pltpu.make_async_copy(src, dst, isem.at[i]) for i, (src, dst) in enumerate(loads)]
    for c in copies:
        c.start()
    small_in = [pltpu.make_async_copy(src, dst, ssem.at[i]) for i, (src, dst) in enumerate(((dgain, dgv), (loss.at[0:1], lossv)))]
    small_out = [pltpu.make_async_copy(src, dst, ssem.at[2 + i]) for i, (src, dst) in enumerate(((dgv, g_gain.at[0]), (lossv, loss_out)))]
    for c in small_in:
        c.start()

    def tile(g, r, c):
        return g.at[0, pl.ds(pl.multiple_of(r * D, D), D), pl.ds(pl.multiple_of(c * T, T), T)]

    def section(base, left, right, g, rows, cols):
        def step(i, carry):
            slot = lax.rem(base + i, STAGES)
            r, c = lax.div(i, cols), lax.rem(i, cols)

            @pl.when(base + i >= STAGES)
            def _():
                pltpu.make_async_copy(stage.at[slot], tile(g_out, 0, 0), osem.at[slot]).wait()
            a = left[:, pl.ds(pl.multiple_of(r * D, D), D)]
            stage[slot] = dot_tn(a, right[:, pl.ds(pl.multiple_of(c * T, T), T)])
            pltpu.make_async_copy(stage.at[slot], tile(g, r, c), osem.at[slot]).start()
            return carry
        lax.fori_loop(0, rows * cols, step, 0)
        return base + rows * cols

    base = 0
    for pair, left, right, g in ((0, attv, dhmv, g_out), (2, actv, dhov, g_down), (4, n2v, duv, g_up), (6, n1v, dqkvv, g_qkv)):
        if pair != 2:
            copies[pair].wait()
            copies[pair + 1].wait()
        else:
            copies[2].wait()
            copies[3].wait()
        base = section(base, left, right, g, left.shape[1] // D, right.shape[1] // T)
    for a, b in zip(small_in, small_out):
        a.wait()
        b.start()
    for b in small_out:
        b.wait()
    for slot in range(STAGES):
        pltpu.make_async_copy(stage.at[slot], tile(g_out, 0, 0), osem.at[slot]).wait()


def weight_grads(n1, dqkv, att, dhm, n2, du, act, dho, loss, dgain):
    D = n1.shape[1]
    hbm = pl.BlockSpec(memory_space=pl.ANY)
    ins = (n1, dqkv, att, dhm, n2, du, act, dho)
    shapes = ((D, dqkv.shape[1]), (D, D), (D, du.shape[1]), (act.shape[1], D))
    dma = pltpu.SemaphoreType.DMA
    return pl.pallas_call(
        wgrad_kernel,
        out_shape=[jax.ShapeDtypeStruct((1,) + sh, F32) for sh in shapes + (dgain.shape,)] + [jax.ShapeDtypeStruct((1, 128), F32)],
        in_specs=[hbm] * 10,
        out_specs=[hbm] * 6,
        scratch_shapes=[pltpu.VMEM(a.shape, BF) for a in ins] + [pltpu.VMEM((STAGES, D, D // 2), F32), pltpu.VMEM(dgain.shape, F32), pltpu.VMEM((1, 128), F32),
                                                                dma((8,)), dma((STAGES,)), dma((4,))],
        compiler_params=pltpu.CompilerParams(vmem_limit_bytes=60 * 2 ** 20),
        name='weight_grads',
    )(*ins, loss, dgain)


def solution(mesh):
    stages = mesh.shape['stage']

    def per_device(x, y, w_qkv, w_out, w_up, w_down, norm_gain):
        loss, dgain, n1, att, n2, act, du, dqkv, dhm, dho, _ = run_pipeline(stages, x, y, w_qkv, w_out, w_up, w_down, norm_gain)
        g_qkv, g_out, g_up, g_down, g_gain, loss = weight_grads(n1, dqkv, att, dhm, n2, du, act, dho, loss, dgain)
        return loss[0, :1], g_qkv, g_out, g_up, g_down, g_gain

    weight_spec = P('stage')
    grad_spec = P(('data', 'stage'))
    return jax.shard_map(per_device, mesh=mesh, in_specs=(P('data'), P('data')) + (weight_spec,) * 5,
                         out_specs=(P('data'),) + (grad_spec,) * 5, check_vma=False)
```

```python
import functools
import math

import jax
import jax.numpy as jnp
from jax import lax
from jax.experimental import pallas as pl
from jax.experimental.pallas import tpu as pltpu
from jax.sharding import PartitionSpec as P

MESH = pl.DeviceIdType.MESH
BF = jnp.bfloat16
F32 = jnp.float32
HEAD_DIM = 64
ROWS = 128
RING = 6
CHUNKS = 12
STAGES = 5
EPS = 1e-6
GELU_C = math.sqrt(2.0 / math.pi)
GELU_A = 0.044715
LOG2E = math.log2(math.e)


def dot_nn(a, b):
    return jnp.dot(a, b, preferred_element_type=F32)


def dot_nt(a, b):
    return lax.dot_general(a, b, (((1,), (1,)), ((), ())), preferred_element_type=F32)


def dot_tn(a, b):
    return lax.dot_general(a, b, (((0,), (0,)), ((), ())), preferred_element_type=F32)


def norm_stats(h_bf):
    h = h_bf.astype(F32)
    inv = lax.rsqrt(jnp.mean(h * h, axis=-1, keepdims=True) + EPS)
    return h, inv


def norm_grad(dn, h_bf, gain):
    h, inv = norm_stats(h_bf)
    hhat = h * inv
    dgain = jnp.sum(dn * hhat, axis=0, keepdims=True)
    dhhat = dn * gain
    corr = jnp.mean(dhhat * hhat, axis=-1, keepdims=True)
    return inv * (dhhat - hhat * corr), dgain


def gelu_parts(u):
    u2 = u * u
    t = jnp.tanh(u * (GELU_C + (GELU_C * GELU_A) * u2))
    return u2, t


def pipeline_kernel(stages, seq, width, x_ref, y_ref, wqkv, wout, wup, wdown, gain_ref,
                    loss_ref, dgain_ref, n1_o, a_o, n2_o, act_o, du_o, dqkv_o, dhm_o, dho_o, wt,
                    ring, hin, hs, hmid, n1, att, n2, qkv, u_buf, act, acc, dho, bias, loss_in,
                    sb0, sb1, pb0, pb1, lse,
                    wsem, esem, tsem, xsem, osem, fs, fr, bs, br, ls, lr):
    me = lax.axis_index('stage')
    data = lax.axis_index('data')
    last = stages - 1
    half = stages // 2
    right = lax.rem(me + 1, stages)
    left = lax.rem(me + stages - 1, stages)
    D = width
    CH = D
    LN = 2 * HEAD_DIM
    pairs = D // LN
    pieces = seq // ROWS
    count = float(seq * width)
    sbuf, pbuf = (sb0, sb1), (pb0, pb1)

    def fetch(kind, j, slot, extra=None):
        cols = pl.ds(pl.multiple_of(j * CH, CH), CH)
        src = {'q': lambda: wqkv.at[0, :, cols], 'o': lambda: wout.at[0], 'u': lambda: wup.at[0, :, cols], 'd': lambda: wdown.at[0, cols, :]}[kind]()
        if extra is None:
            pltpu.make_async_copy(src, ring.at[slot], wsem.at[slot]).start()
        else:
            pltpu.make_async_copy(src, extra.at[slot], esem.at[slot]).start()

    def fetch_bwd(idx):
        slot = lax.rem(idx, RING)
        pltpu.make_async_copy(wt.at[idx], ring.at[slot], wsem.at[slot]).start()

    def arrived(slot):
        pltpu.make_async_copy(wout.at[0], ring.at[slot], wsem.at[slot]).wait()

    def put(idx, p, buf, out):
        return pltpu.make_async_copy(buf, out.at[pl.ds(pl.multiple_of(p * ROWS, ROWS), ROWS)], osem.at[idx, p])

    def fwd_copy(p):
        return pltpu.make_async_remote_copy(src_ref=hs.at[p], dst_ref=hin.at[p], send_sem=fs.at[p], recv_sem=fr.at[p],
                                            device_id=(data, right), device_id_type=MESH)

    def bwd_copy(p):
        return pltpu.make_async_remote_copy(src_ref=hs.at[p], dst_ref=dho.at[p], send_sem=bs.at[p], recv_sem=br.at[p],
                                            device_id=(data, left), device_id_type=MESH)

    def loss_copy():
        return pltpu.make_async_remote_copy(src_ref=loss_in, dst_ref=loss_in, send_sem=ls.at[0], recv_sem=lr.at[0],
                                            device_id=(data, left), device_id_type=MESH)

    def transpose_weights():
        def fetch_any(b):
            slot = lax.rem(b, 3)
            for odd, kind in ((0, 'd'), (1, 'u')):
                @pl.when((b < 8) & (lax.rem(b, 2) == odd))
                def _(kind=kind):
                    fetch(kind, lax.div(b, 2), slot)

            @pl.when(b == 8)
            def _():
                fetch('o', 0, slot)

            @pl.when(b > 8)
            def _():
                fetch('q', b - 9, slot)

        def store(b):
            slot = lax.rem(b, 3)
            return pltpu.make_async_copy(ring.at[slot + 3], wt.at[b], tsem.at[slot])

        fetch_any(0)
        fetch_any(1)

        @pl.loop(0, CHUNKS)
        def _(b):
            slot = lax.rem(b, 3)

            @pl.when(b + 2 < CHUNKS)
            def _():
                fetch_any(b + 2)
            arrived(slot)

            @pl.when(b >= 3)
            def _():
                store(b - 3).wait()

            @pl.loop(0, D // 256)
            def _(r):
                blk = pl.ds(pl.multiple_of(r * 256, 256), 256)
                ring[slot + 3, :, blk] = ring[slot, blk, :].T
            store(b).start()

        @pl.loop(CHUNKS - 3, CHUNKS)
        def _(b):
            store(b).wait()

    def start_fwd(extra):
        for c in range(3):
            fetch('q', c, c)
        fetch('o', 0, 3)
        fetch('u', 0, 4)
        fetch('d', 0, 5)
        for e, (kind, j) in enumerate((('u', 1), ('d', 1), ('u', 2), ('d', 2), ('d', 3))):
            fetch(kind, j, e, extra)

    @pl.when(me == 0)
    def _():
        for p in range(pieces):
            pltpu.make_async_copy(x_ref.at[0, pl.ds(p * ROWS, ROWS)], hin.at[p], xsem.at[p]).start()

    @pl.when(me == last)
    def _():
        for p in range(pieces):
            pltpu.make_async_copy(y_ref.at[0, pl.ds(p * ROWS, ROWS)], dho.at[p], xsem.at[p]).start()

    barrier = pltpu.get_barrier_semaphore()
    for nb in (left, right):
        pl.semaphore_signal(barrier, inc=1, device_id=(data, nb), device_id_type=MESH)
    pl.semaphore_wait(barrier, 2)

    @pl.when(me >= half)
    def _():
        transpose_weights()

    dgain_ref[...] = jnp.zeros_like(dgain_ref)

    @pl.when(me == last)
    def _():
        loss_in[...] = jnp.zeros_like(loss_in)
    gain0 = gain_ref[0, 0:1, :].astype(F32)
    gain1 = gain_ref[0, 1:2, :].astype(F32)
    low = lax.broadcasted_iota(jnp.int32, (ROWS, LN), 1) < HEAD_DIM

    def stack(a):
        zero = jnp.zeros_like(a)
        return jnp.concatenate([jnp.where(low, a, zero), jnp.where(low, zero, a)], axis=0)

    def unstack(a):
        return jnp.where(low, a[:ROWS], a[ROWS:])

    def lanes(i, base=0):
        if isinstance(i, int):
            return pl.ds(i * LN + base, LN)
        return pl.ds(pl.multiple_of(i * LN, LN) + base, LN)

    r = lax.rem(lax.broadcasted_iota(jnp.int32, (2 * ROWS, ROWS), 0), ROWS)
    c = lax.broadcasted_iota(jnp.int32, (2 * ROWS, ROWS), 1)
    bias[...] = jnp.where(c <= r, 0.0, -1e30)

    lane = lax.broadcasted_iota(jnp.int32, (2 * ROWS, 128), 1)

    def masked(s):
        s = s * (HEAD_DIM ** -0.5 * LOG2E)
        keys = s.shape[1]
        if keys > ROWS:
            return jnp.concatenate([s[:, :keys - ROWS], s[:, keys - ROWS:] + bias[...]], axis=1)
        return s + bias[...]

    def by_piece(p, body):
        for k in range(pieces):
            @pl.when(p == k)
            def _(k=k):
                body((k + 1) * ROWS)

    def pair_pipeline(unrolled, first, middle, final):
        first(0, 0)
        if unrolled:
            for i in range(pairs):
                if i + 1 < pairs:
                    first(i + 1, (i + 1) % 2)
                middle(i, i % 2)
                if i > 0:
                    final(i - 1, (i - 1) % 2)
            final(pairs - 1, (pairs - 1) % 2)
            return

        @pl.loop(0, pairs // 2)
        def _(h):
            i = 2 * h
            first(i + 1, 1)
            middle(i, 0)
            final(jnp.maximum(i - 1, 0), 1)
            first(jnp.minimum(i + 2, pairs - 1), 0)
            middle(i + 1, 1)
            final(i, 0)
        final(pairs - 1, 1)

    def fwd_piece(extra, p, carry):
        row0 = pl.multiple_of(p * ROWS, ROWS)
        rows = pl.ds(row0, ROWS)
        w = lax.rem(p, 2)

        @pl.when(p >= 2)
        def _():
            put(0, p - 2, n1.at[w], n1_o).wait()
            put(2, p - 2, n2.at[w], n2_o).wait()
            put(3, p - 2, act.at[w], act_o).wait()

        @pl.when(me == 0)
        def _():
            pltpu.make_async_copy(x_ref.at[0, rows], hin.at[p], xsem.at[p]).wait()

        @pl.when(me > 0)
        def _():
            fwd_copy(p).wait_recv()

        @pl.when(p == 0)
        def _():
            for c in range(3):
                arrived(c)

        turn = (p == pieces - 1) & (me >= half)

        h, inv = norm_stats(hin[p])
        n1[w] = (h * inv * gain0).astype(BF)
        put(0, p, n1.at[w], n1_o).start()

        for c in range(3):
            qkv[rows, c * CH:(c + 1) * CH] = dot_nn(n1[w], ring[c]).astype(BF)

        @pl.when(turn)
        def _():
            for c in range(3):
                fetch_bwd(c)

        def attend(keys):
            def scores(i, b):
                sbuf[b][:, :keys] = dot_nt(stack(qkv[rows, lanes(i)]), qkv[:keys, lanes(i, D)])

            def softmax(i, b):
                s = masked(sbuf[b][:, :keys])
                top = jnp.max(s, axis=-1, keepdims=True)
                e = jnp.exp2(s - top)
                total = jnp.sum(e, axis=-1, keepdims=True)
                lse[p] = jnp.where(lane == i, top + jnp.log2(total), lse[p])
                pbuf[b][:, :keys] = (e * (1.0 / total)).astype(BF)

            def mix(i, b):
                att[p, :, lanes(i)] = unstack(dot_nn(pbuf[b][:, :keys], qkv[:keys, lanes(i, 2 * D)])).astype(BF)

            pair_pipeline(keys == seq, scores, softmax, mix)

        by_piece(p, attend)
        put(1, p, att.at[p], a_o).start()
        arrived(3)
        hmid[p] = (hin[p].astype(F32) + dot_nn(att[p], ring[3])).astype(BF)
        fetch('u', 3, 3)
        h, inv = norm_stats(hmid[p])
        n2[w] = (h * inv * gain1).astype(BF)
        put(2, p, n2.at[w], n2_o).start()

        @pl.when(p == 0)
        def _():
            arrived(4)
            arrived(5)
            for e in range(5):
                pltpu.make_async_copy(wout.at[0], extra.at[e], esem.at[e]).wait()

        def up(j, weight):
            u_buf[rows, j * CH:(j + 1) * CH] = dot_nn(n2[w], weight[...])

        def down(j, weight):
            u = u_buf[rows, j * CH:(j + 1) * CH]
            u2, t = gelu_parts(u)
            act[w, :, j * CH:(j + 1) * CH] = (0.5 * u * (1.0 + t)).astype(BF)
            return dot_nn(act[w, :, j * CH:(j + 1) * CH], weight[...])

        up(0, ring.at[4])
        up(1, extra.at[0])
        acc[...] = hmid[p].astype(F32) + down(0, ring.at[5])
        up(2, extra.at[2])
        acc[...] += down(1, extra.at[1])
        arrived(3)
        up(3, ring.at[3])
        acc[...] += down(2, extra.at[3])
        hs[p] = (acc[...] + down(3, extra.at[4])).astype(BF)

        @pl.when(me < last)
        def _():
            fwd_copy(p).start()

        put(3, p, act.at[w], act_o).start()

        @pl.when(p < pieces - 1)
        def _():
            fetch('o', 0, 3)

        @pl.when(turn)
        def _():
            for b in range(3, RING):
                fetch_bwd(b)

        @pl.when(me == last)
        def _():
            pltpu.make_async_copy(y_ref.at[0, rows], dho.at[p], xsem.at[p]).wait()
            err = hs[p].astype(F32) - dho[p].astype(F32)
            dho[p] = (err / count).astype(BF)
            part = jnp.sum(jnp.sum(err * err, axis=0, keepdims=True), axis=1, keepdims=True)
            loss_in[...] += part * (0.5 / count)
        return carry

    def forward(extra):
        start_fwd(extra)
        lax.fori_loop(0, pieces, functools.partial(fwd_piece, extra), 0)

    pl.run_scoped(forward, pltpu.VMEM((5, D, D), BF))

    @pl.when(me < half)
    def _():
        transpose_weights()
        for b in range(RING):
            fetch_bwd(b)
    def bwd_piece(bufs, t, carry):
        gbuf, dbuf, du, dqkv, dhm, da, dkvt = bufs
        p = pieces - 1 - t
        row0 = pl.multiple_of(p * ROWS, ROWS)
        rows = pl.ds(row0, ROWS)
        w = lax.rem(t, 2)

        @pl.when(t >= 2)
        def _():
            put(4, p + 2, du.at[w], du_o).wait()
            put(5, p + 2, dqkv.at[w], dqkv_o).wait()
            put(6, p + 2, dhm.at[w], dhm_o).wait()

        @pl.when(me < last)
        def _():
            bwd_copy(p).wait_recv()

        @pl.when((me < last) & (t == 0))
        def _():
            loss_copy().wait_recv()

        @pl.when((me > 0) & (t == 0))
        def _():
            loss_copy().start()
        put(7, p, dho.at[p], dho_o).start()

        def fetch_next(idx):
            nxt = idx + RING
            if nxt < CHUNKS:
                fetch_bwd(nxt)
            else:
                @pl.when(t < pieces - 1)
                def _():
                    fetch_bwd(nxt - CHUNKS)

        def back_down(j):
            dbuf[j % 2][...] = dot_nn(dho[p], ring[2 * j % RING])

        def back_up(j):
            cols = slice(j * CH, (j + 1) * CH)
            u = u_buf[rows, cols]
            u2, th = gelu_parts(u)
            slope = 0.5 * (1.0 + th) + (0.5 * u) * (1.0 - th * th) * (GELU_C + (3.0 * GELU_C * GELU_A) * u2)
            du[w, :, cols] = (dbuf[j % 2][...] * slope).astype(BF)
            return dot_nn(du[w, :, cols], ring[(2 * j + 1) % RING])

        for idx in range(3):
            arrived(idx)
        back_down(0)
        back_down(1)
        acc[...] = back_up(0)
        for idx in range(3):
            fetch_next(idx)
        for idx in range(3, 6):
            arrived(idx)
        back_down(2)
        acc[...] += back_up(1) + back_up(2)
        for idx in range(3, 6):
            fetch_next(idx)
        for idx in range(6, 8):
            arrived(idx % RING)
        back_down(3)
        acc[...] += back_up(3)
        for idx in range(6, 8):
            fetch_next(idx)

        put(4, p, du.at[w], du_o).start()
        dh, dg = norm_grad(acc[...], hmid[p], gain1)
        dgain_ref[1:2, :] += dg
        dhm[w] = (dho[p].astype(F32) + dh).astype(BF)
        put(6, p, dhm.at[w], dhm_o).start()
        arrived(8 % RING)
        da[...] = dot_nn(dhm[w], ring[8 % RING]).astype(BF)
        fetch_next(8)

        def attend(keys):
            scale = HEAD_DIM ** -0.5

            def slopes(i, b):
                prod = da[:, lanes(i)].astype(F32) * att[p, :, lanes(i)].astype(F32)
                both = jnp.concatenate([jnp.where(low, prod, 0.0), jnp.where(low, 0.0, prod)], axis=0)
                delta = jnp.sum(both, axis=-1, keepdims=True)
                norm = jnp.sum(jnp.where(lane == i, lse[p], 0.0), axis=-1, keepdims=True)
                pr = jnp.exp2(masked(dot_nt(stack(qkv[rows, lanes(i)]), qkv[:keys, lanes(i, D)])) - norm)
                pbuf[b][:, :keys] = pr.astype(BF)
                dp = dot_nt(stack(da[:, lanes(i)]), qkv[:keys, lanes(i, 2 * D)])
                gbuf[b][:, :keys] = (pr * (dp - delta)).astype(BF)

            def grads(i, b):
                g = gbuf[b][:, :keys]
                dqkv[w, :, lanes(i)] = (unstack(dot_nn(g, qkv[:keys, lanes(i, D)])) * scale).astype(BF)
                dk = dot_tn(stack(qkv[rows, lanes(i)]) * scale, g)
                dv = dot_tn(stack(da[:, lanes(i)]), pbuf[b][:, :keys])
                if keys == seq:
                    dkvt[lanes(i), :] = dk
                    dkvt[lanes(i, D), :] = dv
                else:
                    dkvt[lanes(i), :keys] += dk
                    dkvt[lanes(i, D), :keys] += dv

            slopes(0, 0)
            if keys == seq:
                for i in range(pairs):
                    if i + 1 < pairs:
                        slopes(i + 1, (i + 1) % 2)
                    grads(i, i % 2)
                return

            @pl.loop(0, pairs // 2)
            def _(h):
                slopes(2 * h + 1, 1)
                grads(2 * h, 0)
                slopes(jnp.minimum(2 * h + 2, pairs - 1), 0)
                grads(2 * h + 1, 1)

        by_piece(p, attend)

        @pl.loop(0, 2)
        def _(g):
            for e in range(pairs):
                i = g * pairs + e
                dqkv[w, :, lanes(i, D)] = dkvt[lanes(i), rows].astype(BF).T

        put(5, p, dqkv.at[w], dqkv_o).start()
        for c in range(3):
            arrived((c + 9) % RING)
        dn = dot_nn(dqkv[w, :, 0:CH], ring[9 % RING])
        for c in range(1, 3):
            dn = dn + dot_nn(dqkv[w, :, c * CH:(c + 1) * CH], ring[(c + 9) % RING])
        acc[...] = dn
        for c in range(3):
            fetch_next(c + 9)
        dh, dg = norm_grad(acc[...], hin[p], gain0)
        dgain_ref[0:1, :] += dg

        @pl.when(me > 0)
        def _():
            @pl.when(me < last)
            def _():
                fwd_copy(p).wait_send()
            hs[p] = (dhm[w].astype(F32) + dh).astype(BF)
            bwd_copy(p).start()
        return carry

    def backward(gb0, gb1, db0, db1, du, dqkv, dhm, da, dkvt):
        bufs = ((gb0, gb1), (db0, db1), du, dqkv, dhm, da, dkvt)
        lax.fori_loop(0, pieces, functools.partial(bwd_piece, bufs), 0)
        for e in range(2):
            put(4, e, du.at[1 - e], du_o).wait()
            put(5, e, dqkv.at[1 - e], dqkv_o).wait()
            put(6, e, dhm.at[1 - e], dhm_o).wait()

    tight, part = pltpu.VMEM((2 * ROWS, seq), BF), pltpu.VMEM((ROWS, D), F32)
    pl.run_scoped(backward, tight, tight, part, part,
                  pltpu.VMEM((2, ROWS, 4 * CH), BF), pltpu.VMEM((2, ROWS, 3 * CH), BF), pltpu.VMEM((2, ROWS, D), BF),
                  pltpu.VMEM((ROWS, D), BF), pltpu.VMEM((2 * D, seq), F32))
    loss_ref[...] = loss_in[...]

    for p in range(pieces):
        put(1, p, att.at[p], a_o).wait()
        put(7, p, dho.at[p], dho_o).wait()

        @pl.when(me == 0)
        def _():
            fwd_copy(p).wait_send()

        @pl.when(me > 0)
        def _():
            bwd_copy(p).wait_send()
    for e in range(2):
        p = pieces - 2 + e
        put(0, p, n1.at[e], n1_o).wait()
        put(2, p, n2.at[e], n2_o).wait()
        put(3, p, act.at[e], act_o).wait()

    @pl.when(me > 0)
    def _():
        loss_copy().wait_send()


def run_pipeline(stages, x, y, w_qkv, w_out, w_up, w_down, gain):
    seq, width = x.shape[1], x.shape[2]
    ffn = w_up.shape[2]
    pieces = seq // ROWS
    hbm = pl.BlockSpec(memory_space=pl.ANY)
    vmem = pl.BlockSpec(memory_space=pltpu.VMEM)
    V = pltpu.VMEM
    full = V((pieces, ROWS, width), BF)
    two = V((2, ROWS, width), BF)
    wide = V((2 * ROWS, seq), F32)
    tight = V((2 * ROWS, seq), BF)
    widths = (width, width, width, ffn, ffn, 3 * width, width, width)
    outs = [jax.ShapeDtypeStruct((8, 128), F32), jax.ShapeDtypeStruct((2, width), F32)]
    outs += [jax.ShapeDtypeStruct((seq, w), BF) for w in widths]
    outs += [jax.ShapeDtypeStruct((CHUNKS, width, width), BF)]
    dma = pltpu.SemaphoreType.DMA
    return pl.pallas_call(
        functools.partial(pipeline_kernel, stages, seq, width),
        out_shape=outs,
        in_specs=[hbm] * 6 + [vmem],
        out_specs=[vmem, vmem] + [hbm] * 9,
        scratch_shapes=[
            V((RING, width, width), BF),
            full, full, full,
            two, full, two,
            V((seq, 3 * width), BF),
            V((seq, ffn), F32),
            V((2, ROWS, ffn), BF),
            V((ROWS, width), F32),
            full,
            V((2 * ROWS, ROWS), F32), V((8, 128), F32),
            wide, wide, tight, tight, V((pieces, 2 * ROWS, 128), F32),
            dma((RING,)), dma((5,)), dma((3,)), dma((pieces,)), dma((8, pieces)),
            dma((pieces,)), dma((pieces,)), dma((pieces,)), dma((pieces,)), dma((1,)), dma((1,)),
        ],
        compiler_params=pltpu.CompilerParams(collective_id=0, has_side_effects=True, vmem_limit_bytes=67043328),
        name='pipeline',
    )(x, y, w_qkv, w_out, w_up, w_down, gain)


def wgrad_kernel(n1, dqkv, att, dhm, n2, du, act, dho, loss, dgain, g_qkv, g_out, g_up, g_down, g_gain, loss_out,
                 n1v, dqkvv, attv, dhmv, n2v, duv, actv, dhov, stage, dgv, lossv, isem, osem, ssem):
    D = n1.shape[1]
    T = stage.shape[2]
    loads = ((att, attv), (dhm, dhmv), (dho, dhov), (act, actv), (n2, n2v), (du, duv), (n1, n1v), (dqkv, dqkvv))
    copies = [pltpu.make_async_copy(src, dst, isem.at[i]) for i, (src, dst) in enumerate(loads)]
    for c in copies:
        c.start()
    small_in = [pltpu.make_async_copy(src, dst, ssem.at[i]) for i, (src, dst) in enumerate(((dgain, dgv), (loss.at[0:1], lossv)))]
    small_out = [pltpu.make_async_copy(src, dst, ssem.at[2 + i]) for i, (src, dst) in enumerate(((dgv, g_gain.at[0]), (lossv, loss_out)))]
    for c in small_in:
        c.start()

    def tile(g, r, c):
        return g.at[0, pl.ds(pl.multiple_of(r * D, D), D), pl.ds(pl.multiple_of(c * T, T), T)]

    def section(base, left, right, g, rows, cols):
        def step(i, carry):
            slot = lax.rem(base + i, STAGES)
            r, c = lax.div(i, cols), lax.rem(i, cols)

            @pl.when(base + i >= STAGES)
            def _():
                pltpu.make_async_copy(stage.at[slot], tile(g_out, 0, 0), osem.at[slot]).wait()
            a = left[:, pl.ds(pl.multiple_of(r * D, D), D)]
            stage[slot] = dot_tn(a, right[:, pl.ds(pl.multiple_of(c * T, T), T)])
            pltpu.make_async_copy(stage.at[slot], tile(g, r, c), osem.at[slot]).start()
            return carry
        lax.fori_loop(0, rows * cols, step, 0)
        return base + rows * cols

    base = 0
    for pair, left, right, g in ((0, attv, dhmv, g_out), (2, actv, dhov, g_down), (4, n2v, duv, g_up), (6, n1v, dqkvv, g_qkv)):
        if pair != 2:
            copies[pair].wait()
            copies[pair + 1].wait()
        else:
            copies[2].wait()
            copies[3].wait()
        base = section(base, left, right, g, left.shape[1] // D, right.shape[1] // T)
    for a, b in zip(small_in, small_out):
        a.wait()
        b.start()
    for b in small_out:
        b.wait()
    for slot in range(STAGES):
        pltpu.make_async_copy(stage.at[slot], tile(g_out, 0, 0), osem.at[slot]).wait()


def weight_grads(n1, dqkv, att, dhm, n2, du, act, dho, loss, dgain):
    D = n1.shape[1]
    hbm = pl.BlockSpec(memory_space=pl.ANY)
    ins = (n1, dqkv, att, dhm, n2, du, act, dho)
    shapes = ((D, dqkv.shape[1]), (D, D), (D, du.shape[1]), (act.shape[1], D))
    dma = pltpu.SemaphoreType.DMA
    return pl.pallas_call(
        wgrad_kernel,
        out_shape=[jax.ShapeDtypeStruct((1,) + sh, F32) for sh in shapes + (dgain.shape,)] + [jax.ShapeDtypeStruct((1, 128), F32)],
        in_specs=[hbm] * 10,
        out_specs=[hbm] * 6,
        scratch_shapes=[pltpu.VMEM(a.shape, BF) for a in ins] + [pltpu.VMEM((STAGES, D, D // 2), F32), pltpu.VMEM(dgain.shape, F32), pltpu.VMEM((1, 128), F32),
                                                                dma((8,)), dma((STAGES,)), dma((4,))],
        compiler_params=pltpu.CompilerParams(vmem_limit_bytes=60 * 2 ** 20),
        name='weight_grads',
    )(*ins, loss, dgain)


def solution(mesh):
    stages = mesh.shape['stage']

    def per_device(x, y, w_qkv, w_out, w_up, w_down, norm_gain):
        loss, dgain, n1, att, n2, act, du, dqkv, dhm, dho, _ = run_pipeline(stages, x, y, w_qkv, w_out, w_up, w_down, norm_gain)
        g_qkv, g_out, g_up, g_down, g_gain, loss = weight_grads(n1, dqkv, att, dhm, n2, du, act, dho, loss, dgain)
        return loss[0, :1], g_qkv, g_out, g_up, g_down, g_gain

    weight_spec = P('stage')
    grad_spec = P(('data', 'stage'))
    return jax.shard_map(per_device, mesh=mesh, in_specs=(P('data'), P('data')) + (weight_spec,) * 5,
                         out_specs=(P('data'),) + (grad_spec,) * 5, check_vma=False)
```
